32 devices in a mesh: groups: 2 (over y), seq: 16 (over z, x, core).
Axes of the slice: x: 2, y: 2, z: 4, core: 2. Of those that a mesh axis runs over, the one named last changes fastest.
Arguments:
- queries: bfloat16 [8192, 4096], P(('groups', 'seq')), parts along dimension 0
- new_keys: bfloat16 [8192, 1024], P(('groups', 'seq')), parts along dimension 0
- new_values: bfloat16 [8192, 1024], P(('groups', 'seq')), parts along dimension 0, may hold values from -6 to 6
- pool_keys: bfloat16 [672, 16, 1024], P(('groups', 'seq')), parts along dimension 0, may hold values from -10 to 10
- pool_values: bfloat16 [672, 16, 1024], P(('groups', 'seq')), parts along dimension 0, may hold values from -6 to 6
- prefix_len: int32 [32], P(('groups', 'seq')), parts along dimension 0, may hold values from 1 to 80
- new_len: int32 [32], P(('groups', 'seq')), parts along dimension 0, may hold values from 128 to 256
- page_holder: int32 [32, 5], P(('groups', 'seq')), parts along dimension 0, may hold values from 0 to 15, as said below
- page_slot: int32 [32, 5], P(('groups', 'seq')), parts along dimension 0, may hold values from 0 to 20, as said below
- new_holder: int32 [32, 16], P(('groups', 'seq')), parts along dimension 0, may hold values from 0 to 15, as said below
- new_slot: int32 [32, 16], P(('groups', 'seq')), parts along dimension 0, may hold values from 0 to 20
Outputs:
- attention_out: bfloat16 [8192, 4096], P(('groups', 'seq')), parts along dimension 0
- pool_keys_out: bfloat16 [672, 16, 1024], P(('groups', 'seq')), parts along dimension 0
- pool_values_out: bfloat16 [672, 16, 1024], P(('groups', 'seq')), parts along dimension 0
The draws below stay inside these ranges and needn't reach their ends.
There are 2 independent parts, one for each index of `groups`. The reference program is written for one: setup_inputs(seed, part) draws one part's arguments, and reference() takes and returns one part's arrays. A program takes and returns all parts, laid end to end along the dimension named above; each array names one. Nothing has to cross between parts.
Inputs may be any that keep to these rules, and one draw needn't show every extreme that they name: `page_holder`: the 5 pages named for one conversation lie on distinct devices. No pool slot is named twice by page_slot and new_slot together, and no slot named by new_slot is named by page_slot. `new_holder`: the 16 pages of one conversation's new turn go to distinct devices.
All inputs are finite; a program needn't handle non-finite values.
Results may differ from the reference program's by a relative error of at most 0.0027.
Values may be sent and summed in bfloat16 or wider, within the bound.
No kernel may reach another device: no remote copies, remote signals or barrier semaphores. Data moves between devices by JAX's collectives and lax.ppermute only.
A program may use at most 128 MiB of HBM per device.

```python
import math
import jax
import jax.numpy as jnp
from jax import lax

HEADS = 32
KV_HEADS = 8
HEAD = 128
SPAN = 256
PAGE = 16
KVW = 1024
MAXPRE = 5
NEWP = 16
POOL = 21
TOKENS = 4096
SLOTS = 336
N_SEQ = 16


def attention_draws(key):
    base_key = jax.random.fold_in(key, 11)
    query_key, key_key = jax.random.split(base_key)
    keys_all = 1.7 * jax.random.normal(key_key, (N_SEQ, SPAN, KV_HEADS, HEAD), jnp.float32)
    queries_all = 1.7 * jax.random.normal(query_key, (N_SEQ, SPAN, HEADS, HEAD), jnp.float32)
    return (queries_all.reshape(N_SEQ * SPAN, HEADS * HEAD), keys_all.reshape(N_SEQ * SPAN, KV_HEADS * HEAD))


def draw_queries(key, part):
    return attention_draws(key)[0].astype(jnp.bfloat16)


def draw_new_keys(key, part):
    return attention_draws(key)[1].astype(jnp.bfloat16)


def block_tables(key):
    base_key = jax.random.fold_in(key, 29)
    key_first, key_second, key_third = jax.random.split(base_key, 3)
    order_pre = jax.random.permutation(key_first, N_SEQ).astype(jnp.int32)
    order_new = jax.random.permutation(key_second, N_SEQ).astype(jnp.int32)
    place_pre = jnp.argsort(order_pre).astype(jnp.int32)
    place_new = jnp.argsort(order_new).astype(jnp.int32)
    slot_keys = jax.random.split(key_third, N_SEQ)
    slot_order = jax.vmap(lambda single: jax.random.permutation(single, POOL))(slot_keys).astype(jnp.int32)
    page_ids = jnp.arange(MAXPRE, dtype=jnp.int32)
    fresh_ids = jnp.arange(NEWP, dtype=jnp.int32)
    page_holder = order_pre[(place_pre[:, None] + 1 + page_ids[None, :]) % N_SEQ]
    page_slot = slot_order[page_holder, jnp.broadcast_to(page_ids[None, :], page_holder.shape)]
    new_holder = order_new[(place_new[:, None] + 1 + fresh_ids[None, :]) % N_SEQ]
    new_slot = slot_order[new_holder, jnp.broadcast_to(MAXPRE + fresh_ids[None, :], new_holder.shape)]
    return (page_holder.astype(jnp.int32), page_slot.astype(jnp.int32), new_holder.astype(jnp.int32), new_slot.astype(jnp.int32))


def draw_page_holder(key, part):
    return block_tables(key)[0]


def draw_page_slot(key, part):
    return block_tables(key)[1]


def draw_new_holder(key, part):
    return block_tables(key)[2]


def draw_new_slot(key, part):
    return block_tables(key)[3]


def place_ends(entries, stream_key, low, largest):
    extent = entries.shape
    place = [jax.random.randint(jax.random.fold_in(stream_key, axis), (), 0, extent[axis]) for axis in range(len(extent))]
    entries = entries.at[tuple(place)].set(low)
    longest = extent.index(max(extent))
    place[longest] = (place[longest] + 1) % extent[longest]
    return entries.at[tuple(place)].set(largest)


def level_of(own_key, shape, shards, smallest, largest):
    level = 1.0
    for position, parts in shards:
        steps = jax.random.uniform(jax.random.fold_in(jax.random.fold_in(own_key, 6), position), (parts,), jnp.float32, smallest / len(shards), largest / len(shards))
        level = level * jnp.repeat(jnp.exp(steps), shape[position] // parts).reshape((-1,) + (1,) * (len(shape) - 1 - position))
    return level


def bell_draw(own_key, dims, width, limit, pieces=(), kind=jnp.bfloat16):
    drawn = jax.random.normal(own_key, dims, jnp.float32) * width
    if len(pieces) > 0:
        drawn = level_of(own_key, dims, pieces, -0.22, 0.18) * drawn
    return jnp.clip(drawn, min=-limit, max=limit).astype(kind)


def setup_inputs(seed: int = 0, part: int = 0) -> dict:
    key_list = jax.random.split(jax.random.key(seed), 12)
    part_splits = jax.random.split(jax.random.fold_in(key_list[11], part), 12)
    return {
        "queries": draw_queries(jax.random.fold_in(jax.random.fold_in(key_list[11], part), 71), part),
        "new_keys": draw_new_keys(jax.random.fold_in(jax.random.fold_in(key_list[11], part), 71), part),
        "new_values": bell_draw(part_splits[2], (TOKENS, KVW), 1.0, 6.0, ((0, 16),)),
        "pool_keys": bell_draw(part_splits[3], (SLOTS, PAGE, KVW), 1.7, 10.0, ((0, 16),)),
        "pool_values": bell_draw(part_splits[4], (SLOTS, PAGE, KVW), 1.0, 6.0, ((0, 16),)),
        "prefix_len": place_ends(jax.random.randint(part_splits[5], (N_SEQ,), 1, MAXPRE * PAGE + 1), jax.random.fold_in(part_splits[5], 1), 1, MAXPRE * PAGE).astype(jnp.int32),
        "new_len": place_ends(jax.random.randint(part_splits[6], (N_SEQ,), SPAN // 2, SPAN + 1), jax.random.fold_in(part_splits[6], 1), SPAN // 2, SPAN).astype(jnp.int32),
        "page_holder": draw_page_holder(jax.random.fold_in(jax.random.fold_in(key_list[11], part), 71), part),
        "page_slot": draw_page_slot(jax.random.fold_in(jax.random.fold_in(key_list[11], part), 71), part),
        "new_holder": draw_new_holder(jax.random.fold_in(jax.random.fold_in(key_list[11], part), 71), part),
        "new_slot": draw_new_slot(jax.random.fold_in(jax.random.fold_in(key_list[11], part), 71), part),
    }


def attend(query_rows, prefix_keys, prefix_values, fresh_keys, fresh_values, prefix_tokens, fresh_tokens):
    group_size = HEADS // KV_HEADS
    scaling = 1.0 / math.sqrt(HEAD)
    key_rows = prefix_keys.shape[0]
    prefix_live = jnp.arange(key_rows, dtype=jnp.int32) < prefix_tokens
    token_pos = jnp.arange(SPAN, dtype=jnp.int32)
    fresh_live = (token_pos[None, :] <= token_pos[:, None]) & (token_pos[None, :] < fresh_tokens)
    blocks = []
    for head_group in range(KV_HEADS):
        first_col = head_group * group_size * HEAD
        query_block = query_rows[:, first_col:first_col + group_size * HEAD].reshape(SPAN, group_size, HEAD).astype(jnp.float32)
        key_first = head_group * HEAD
        prefix_key_slice = prefix_keys[:, key_first:key_first + HEAD].astype(jnp.float32)
        prefix_value_slice = prefix_values[:, key_first:key_first + HEAD].astype(jnp.float32)
        fresh_key_slice = fresh_keys[:, key_first:key_first + HEAD].astype(jnp.float32)
        fresh_value_slice = fresh_values[:, key_first:key_first + HEAD].astype(jnp.float32)
        prefix_scores = jnp.einsum('tgd,kd->tgk', query_block, prefix_key_slice, precision=lax.Precision.HIGHEST) * scaling
        fresh_scores = jnp.einsum('tgd,kd->tgk', query_block, fresh_key_slice, precision=lax.Precision.HIGHEST) * scaling
        prefix_scores = jnp.where(prefix_live[None, None, :], prefix_scores, -jnp.inf)
        fresh_scores = jnp.where(fresh_live[:, None, :], fresh_scores, -jnp.inf)
        row_top = jnp.maximum(lax.optimization_barrier(jnp.max(prefix_scores, axis=-1)), lax.optimization_barrier(jnp.max(fresh_scores, axis=-1)))[..., None]
        prefix_weights = jnp.exp(prefix_scores - row_top)
        fresh_weights = jnp.exp(fresh_scores - row_top)
        weight_sum = lax.optimization_barrier(jnp.sum(prefix_weights, axis=-1)) + lax.optimization_barrier(jnp.sum(fresh_weights, axis=-1))
        prefix_round = lax.optimization_barrier(prefix_weights.astype(jnp.bfloat16)).astype(jnp.float32)
        fresh_round = lax.optimization_barrier(fresh_weights.astype(jnp.bfloat16)).astype(jnp.float32)
        weighted = jnp.einsum('tgk,kd->tgd', prefix_round, prefix_value_slice, precision=lax.Precision.HIGHEST)
        weighted = weighted + jnp.einsum('tgk,kd->tgd', fresh_round, fresh_value_slice, precision=lax.Precision.HIGHEST)
        blocks.append((weighted / weight_sum[..., None]).reshape(SPAN, group_size * HEAD))
    joined = jnp.concatenate(blocks, axis=1)
    row_live = (token_pos < fresh_tokens)[:, None]
    return jnp.where(row_live, joined, 0.0).astype(jnp.bfloat16)

def reference(queries, new_keys, new_values, pool_keys, pool_values, prefix_len, new_len, page_holder, page_slot, new_holder, new_slot):
    kv_width = KV_HEADS * HEAD

    def conversation(device):
        page_rows = (page_holder[device] * POOL + page_slot[device]).astype(jnp.int32)
        prefix_keys = jnp.take(pool_keys, page_rows, axis=0).reshape(MAXPRE * PAGE, kv_width)
        prefix_values = jnp.take(pool_values, page_rows, axis=0).reshape(MAXPRE * PAGE, kv_width)
        row_start = (device * SPAN).astype(jnp.int32)
        query_rows = lax.dynamic_slice_in_dim(queries, row_start, SPAN, 0)
        fresh_keys = lax.dynamic_slice_in_dim(new_keys, row_start, SPAN, 0)
        fresh_values = lax.dynamic_slice_in_dim(new_values, row_start, SPAN, 0)
        return attend(query_rows, prefix_keys, prefix_values, fresh_keys, fresh_values, prefix_len[device], new_len[device])
    outputs = lax.map(conversation, jnp.arange(N_SEQ, dtype=jnp.int32))
    attention_out = outputs.reshape(N_SEQ * SPAN, HEADS * HEAD)
    token_pos = jnp.arange(N_SEQ * SPAN, dtype=jnp.int32) % SPAN
    row_keep = (token_pos < jnp.repeat(new_len, SPAN))[:, None]
    kept_keys = jnp.where(row_keep, new_keys, 0).reshape(N_SEQ * NEWP, PAGE, kv_width)
    kept_values = jnp.where(row_keep, new_values, 0).reshape(N_SEQ * NEWP, PAGE, kv_width)
    targets = (new_holder * POOL + new_slot).reshape(-1).astype(jnp.int32)
    pool_keys_out = pool_keys.at[targets].set(kept_keys)
    pool_values_out = pool_values.at[targets].set(kept_values)
    return (attention_out, pool_keys_out, pool_values_out)
```

```python
import functools
import math

import jax
import jax.numpy as jnp
from jax import lax
from jax.experimental import pallas as pl
from jax.experimental.pallas import tpu as pltpu
from jax.sharding import PartitionSpec as P


HEADS = 32
KV_HEADS = 8
HEAD = 128


def score_block(query_block, key_slice, scaling):
    return (
        jnp.einsum("tgd,kd->tgk", query_block, key_slice, preferred_element_type=jnp.float32)
        * scaling
    )


def fresh_scores_all(queries, new_keys, fresh_live, scaling):
    group_size = HEADS // KV_HEADS
    span_rows = queries.shape[0]
    fresh_parts = []
    for head_group in range(KV_HEADS):
        first_col = head_group * group_size * HEAD
        query_block = queries[:, first_col : first_col + group_size * HEAD].reshape(
            span_rows, group_size, HEAD
        )
        key_slice = new_keys[:, head_group * HEAD : (head_group + 1) * HEAD]
        scores = score_block(query_block, key_slice, scaling)
        fresh_parts.append(jnp.where(fresh_live[:, None, :], scores, -jnp.inf))
    return fresh_parts


def general_shards(
    queries,
    new_keys,
    new_values,
    pool_keys,
    pool_values,
    prefix_len,
    new_len,
    page_holder,
    page_slot,
    new_holder,
    new_slot,
):
    devices = lax.axis_size("seq")
    pool_count = pool_keys.shape[0]
    page_rows = pool_keys.shape[1]
    kv_width = pool_keys.shape[2]
    span_rows = queries.shape[0]
    fresh_pages = span_rows // page_rows
    prefix_pages = page_holder.shape[1]
    group_size = HEADS // KV_HEADS
    scaling = 1.0 / math.sqrt(HEAD)
    peer_ids = jnp.arange(devices, dtype=jnp.int32)
    prefix_tokens = prefix_len[0]
    fresh_tokens = new_len[0]
    holders = page_holder[0]
    page_live = jnp.arange(prefix_pages, dtype=jnp.int32) * page_rows < prefix_tokens
    wanted = (holders[None, :] == peer_ids[:, None]) & page_live[None, :]
    request = jnp.sum(jnp.where(wanted, page_slot[0][None, :] + 1, 0), axis=1)
    token_pos = jnp.arange(span_rows, dtype=jnp.int32)
    row_keep = (token_pos < fresh_tokens)[:, None]
    fresh_live = (token_pos[None, :] <= token_pos[:, None]) & (token_pos[None, :] < fresh_tokens)
    kept_keys = jnp.where(row_keep, new_keys, 0).reshape(fresh_pages, page_rows * kv_width)
    kept_values = jnp.where(row_keep, new_values, 0).reshape(fresh_pages, page_rows * kv_width)
    target_hot = new_holder[0][None, :] == peer_ids[:, None]
    hot_matrix = target_hot.astype(jnp.bfloat16)
    out_keys = jnp.dot(hot_matrix, kept_keys, preferred_element_type=jnp.float32).astype(
        jnp.bfloat16
    )
    out_values = jnp.dot(hot_matrix, kept_values, preferred_element_type=jnp.float32).astype(
        jnp.bfloat16
    )
    out_slots = jnp.sum(jnp.where(target_hot, new_slot[0][None, :] + 1, 0), axis=1)
    slot_column = out_slots.astype(jnp.bfloat16)[:, None]
    incoming = (
        lax.all_to_all(
            request.astype(jnp.bfloat16)[:, None], "seq", split_axis=0, concat_axis=0, tiled=True
        ),
        lax.all_to_all(out_keys, "seq", split_axis=0, concat_axis=0, tiled=True),
        lax.all_to_all(out_values, "seq", split_axis=0, concat_axis=0, tiled=True),
        lax.all_to_all(slot_column, "seq", split_axis=0, concat_axis=0, tiled=True),
    )
    asked_slots = incoming[0][:, 0].astype(jnp.int32)
    returned = (incoming[1], incoming[2], incoming[3][:, 0].astype(jnp.int32))
    chosen = jnp.maximum(asked_slots - 1, 0)
    sending = (asked_slots > 0)[:, None, None]
    send_keys = jnp.where(sending, jnp.take(pool_keys, chosen, axis=0), 0)
    send_values = jnp.where(sending, jnp.take(pool_values, chosen, axis=0), 0)
    received_keys, received_values = (
        lax.all_to_all(send_keys, "seq", split_axis=0, concat_axis=0, tiled=True),
        lax.all_to_all(send_values, "seq", split_axis=0, concat_axis=0, tiled=True),
    )
    prefix_keys = jnp.take(received_keys, holders, axis=0).reshape(
        prefix_pages * page_rows, kv_width
    )
    prefix_values = jnp.take(received_values, holders, axis=0).reshape(
        prefix_pages * page_rows, kv_width
    )
    prefix_live = jnp.arange(prefix_pages * page_rows, dtype=jnp.int32) < prefix_tokens
    fresh_parts = fresh_scores_all(queries, new_keys, fresh_live, scaling)
    blocks = []
    for head_group in range(KV_HEADS):
        first_col = head_group * group_size * HEAD
        query_block = queries[:, first_col : first_col + group_size * HEAD].reshape(
            span_rows, group_size, HEAD
        )
        key_first = head_group * HEAD
        prefix_scores = score_block(
            query_block, prefix_keys[:, key_first : key_first + HEAD], scaling
        )
        prefix_scores = jnp.where(prefix_live[None, None, :], prefix_scores, -jnp.inf)
        fresh_part = fresh_parts[head_group]
        row_top = jnp.maximum(jnp.max(prefix_scores, axis=-1), jnp.max(fresh_part, axis=-1))[
            ..., None
        ]
        prefix_weights = jnp.exp(prefix_scores - row_top)
        fresh_weights = jnp.exp(fresh_part - row_top)
        weight_sum = jnp.sum(prefix_weights, axis=-1) + jnp.sum(fresh_weights, axis=-1)
        weighted = jnp.einsum(
            "tgk,kd->tgd",
            prefix_weights.astype(jnp.bfloat16),
            prefix_values[:, key_first : key_first + HEAD],
            preferred_element_type=jnp.float32,
        )
        weighted = weighted + jnp.einsum(
            "tgk,kd->tgd",
            fresh_weights.astype(jnp.bfloat16),
            new_values[:, key_first : key_first + HEAD],
            preferred_element_type=jnp.float32,
        )
        blocks.append((weighted / weight_sum[..., None]).reshape(span_rows, group_size * HEAD))
    attention_out = jnp.where(row_keep, jnp.concatenate(blocks, axis=1), 0.0).astype(jnp.bfloat16)
    slot_target = jnp.where(returned[2] > 0, returned[2] - 1, pool_count)
    pool_keys_out = pool_keys.at[slot_target].set(
        returned[0].reshape(devices, page_rows, kv_width), mode="drop"
    )
    pool_values_out = pool_values.at[slot_target].set(
        returned[1].reshape(devices, page_rows, kv_width), mode="drop"
    )
    return (attention_out, pool_keys_out, pool_values_out)


SMEM = pl.BlockSpec(memory_space=pltpu.SMEM)
VMEM = pl.BlockSpec(memory_space=pltpu.VMEM)
ANY = pl.BlockSpec(memory_space=pl.ANY)
LOG2E = 1.4426950408889634


def pack_new_kernel(chips, new_holder, new_slot, page_holder, page_slot, new_len, keys, values, *rest):
    outs, table, where_page = rest[:chips], rest[chips], rest[chips + 1]
    me = lax.axis_index("seq")
    chip, core = me // 2, me % 2
    pages = new_holder.shape[1]
    rows = keys.shape[0] // pages
    for i in range(pages):
        where_page[new_holder[0, i]] = i
    devices = table.shape[0]
    row = lax.broadcasted_iota(jnp.int32, table.shape, 0)
    lane = lax.broadcasted_iota(jnp.int32, table.shape, 1)
    entry = jnp.zeros(table.shape, jnp.int32)
    for i in range(pages):
        entry = jnp.where((row == new_holder[0, i]) & (lane == 0), new_slot[0, i], entry)
    for j in range(page_holder.shape[1]):
        entry = jnp.where((row == page_holder[0, j]) & (lane == 1), page_slot[0, j] + 1, entry)
    table[...] = entry
    live = new_len[0]
    token = lax.broadcasted_iota(jnp.int32, (rows, keys.shape[1]), 0)
    for r in range(chips):
        for side in range(2):
            page = where_page[2 * (chip ^ r) + (core ^ side)]
            start = pl.multiple_of(page * rows, rows)
            keep = token + start < live
            outs[r][side, 0] = jnp.where(keep, keys[pl.ds(start, rows), :], 0)
            outs[r][side, 1] = jnp.where(keep, values[pl.ds(start, rows), :], 0)


def pack_prefix_kernel(chips, table, pool_keys, pool_values, own, other):
    me = lax.axis_index("seq")
    chip, core = me // 2, me % 2
    for r in range(chips):
        for side, out in ((0, own), (1, other)):
            slot = jnp.maximum(table[2 * (chip ^ r) + (core ^ side), 1] - 1, 0)
            out[r, 0] = pool_keys[slot]
            out[r, 1] = pool_values[slot]


def merge_kernel(chips, own, got, *outs):
    for r in range(1, chips):
        outs[r - 1][0] = own[r]
        outs[r - 1][1] = got[r]


def exchange_pack_kernel(chips, *refs):
    out = refs[chips]
    for r in range(chips):
        out[r] = refs[r][1]


def scatter_kernel(chips, table, pool_keys, pool_values, *refs):
    near, far = refs[:chips], refs[chips]
    keys_out, values_out = refs[chips + 1], refs[chips + 2]
    taken, sems = refs[chips + 3], refs[chips + 4]
    me = lax.axis_index("seq")
    chip, core = me // 2, me % 2
    slots = pool_keys.shape[0]
    for s in range(slots):
        taken[s] = 0
    count = 0
    waits = []
    for r in range(chips):
        for side in range(2):
            slot = table[2 * (chip ^ r) + (core ^ side), 0]
            taken[slot] = 1
            page = near[r].at[0] if side == 0 else far.at[r]
            for kv, dest in ((0, keys_out), (1, values_out)):
                copy = pltpu.make_async_copy(page.at[kv], dest.at[slot], sems.at[count])
                copy.start()
                waits.append(copy)
                count += 1
    for s in range(slots):
        for kv, (pool, dest) in enumerate(((pool_keys, keys_out), (pool_values, values_out))):

            @pl.when(taken[s] == 0)
            def _(pool=pool, dest=dest, s=s, kv=kv):
                pltpu.make_async_copy(pool.at[s], dest.at[s], sems.at[count + 2 * s + kv]).start()

    for copy in waits:
        copy.wait()
    for s in range(slots):
        for kv, (pool, dest) in enumerate(((pool_keys, keys_out), (pool_values, values_out))):

            @pl.when(taken[s] == 0)
            def _(pool=pool, dest=dest, s=s, kv=kv):
                pltpu.make_async_copy(pool.at[s], dest.at[s], sems.at[count + 2 * s + kv]).wait()


def fresh_kernel(group, new_len, queries, keys, values, partial, stats):
    span = keys.shape[0]
    scale = LOG2E / math.sqrt(HEAD)
    row = lax.broadcasted_iota(jnp.int32, (span, span), 0)
    col = lax.broadcasted_iota(jnp.int32, (span, span), 1)
    visible = (col <= row) & (col < new_len[0])
    lane = lax.broadcasted_iota(jnp.int32, (span, stats.shape[-1]), 1)
    packed = jnp.zeros((span, stats.shape[-1]), jnp.float32)
    for h in range(group):
        scores = lax.dot_general(
            queries[:, h * HEAD : (h + 1) * HEAD],
            keys[...],
            (((1,), (1,)), ((), ())),
            preferred_element_type=jnp.float32,
        )
        scores = jnp.where(visible, scores, -jnp.inf)
        top = jnp.max(scores, axis=1, keepdims=True)
        weights = jnp.exp2((scores - top) * scale)
        total = jnp.sum(weights, axis=1, keepdims=True)
        partial[:, h * HEAD : (h + 1) * HEAD] = jnp.dot(
            weights.astype(jnp.bfloat16), values[...], preferred_element_type=jnp.float32
        )
        packed = jnp.where(lane == h, top, packed)
        packed = jnp.where(lane == group + h, total, packed)
    stats[0] = packed


def prefix_kernel(
    chips, group, holder, prefix_len, new_len, queries, partial, stats, own, got, *refs
):
    near = refs[: chips - 1]
    out, keys, values = refs[chips - 1 :]
    me = lax.axis_index("seq")
    chip, core = me // 2, me % 2
    rows = own.shape[2]
    pages = holder.shape[1]

    @pl.when(pl.program_id(0) == 0)
    def _():
        for j in range(pages):
            source = holder[0, j]
            rel, side = (source // 2) ^ chip, (source % 2) ^ core
            for r in range(chips):
                for s in range(2):

                    @pl.when((rel == r) & (side == s))
                    def _(r=r, s=s, j=j):
                        if r == 0:
                            page = (own if s == 0 else got)[0]
                        else:
                            page = near[r - 1][s]
                        keys[pl.ds(j * rows, rows), :] = page[0]
                        values[pl.ds(j * rows, rows), :] = page[1]

    span = queries.shape[0]
    tokens = pages * rows
    scale = LOG2E / math.sqrt(HEAD)
    col = lax.broadcasted_iota(jnp.int32, (span, tokens), 1)
    visible = col < prefix_len[0]
    live = lax.broadcasted_iota(jnp.int32, (span, HEAD), 0) < new_len[0]
    first = pl.multiple_of(pl.program_id(0) * HEAD, HEAD)
    head_keys = keys[:, pl.ds(first, HEAD)]
    head_values = values[:, pl.ds(first, HEAD)]
    for h in range(group):
        scores = lax.dot_general(
            queries[:, h * HEAD : (h + 1) * HEAD],
            head_keys,
            (((1,), (1,)), ((), ())),
            preferred_element_type=jnp.float32,
        )
        scores = jnp.where(visible, scores, -jnp.inf)
        fresh_top = stats[0, :, h : h + 1]
        fresh_total = stats[0, :, group + h : group + h + 1]
        top = jnp.maximum(jnp.max(scores, axis=1, keepdims=True), fresh_top)
        weights = jnp.exp2((scores - top) * scale)
        fade = jnp.exp2((fresh_top - top) * scale)
        total = jnp.sum(weights, axis=1, keepdims=True) + fresh_total * fade
        weighted = jnp.dot(
            weights.astype(jnp.bfloat16), head_values, preferred_element_type=jnp.float32
        )
        weighted = (weighted + partial[:, h * HEAD : (h + 1) * HEAD] * fade) / total
        out[:, h * HEAD : (h + 1) * HEAD] = jnp.where(live, weighted, 0.0).astype(jnp.bfloat16)


def exchange_shards(
    queries,
    new_keys,
    new_values,
    pool_keys,
    pool_values,
    prefix_len,
    new_len,
    page_holder,
    page_slot,
    new_holder,
    new_slot,
):
    devices = lax.axis_size("seq")
    chips = devices // 2
    group = HEADS // KV_HEADS
    span = queries.shape[0]
    slots, rows, width = pool_keys.shape
    prefix_pages = page_holder.shape[1]
    bf16, f32 = jnp.bfloat16, jnp.float32

    def swap(value, offset):
        return lax.ppermute(value, "seq", [(i, i ^ offset) for i in range(devices)])

    message = jax.ShapeDtypeStruct((2, 2, rows, width), bf16)
    stack = jax.ShapeDtypeStruct((chips, 2, rows, width), bf16)
    *packed, table = pl.pallas_call(
        functools.partial(pack_new_kernel, chips),
        out_shape=[message] * chips + [jax.ShapeDtypeStruct((devices, HEAD), jnp.int32)],
        in_specs=[SMEM] * 5 + [VMEM] * 2,
        out_specs=[VMEM] * (chips + 1),
        scratch_shapes=[pltpu.SMEM((devices,), jnp.int32)],
        name="pack_new",
    )(new_holder, new_slot, page_holder, page_slot, new_len, new_keys, new_values)
    arrived = [None] * chips
    arrived[0] = packed[0]
    for r in range(chips - 1, 0, -1):
        arrived[r] = swap(packed[r], 2 * r)
    table = lax.all_to_all(table, "seq", split_axis=0, concat_axis=0, tiled=True)

    own, other = pl.pallas_call(
        functools.partial(pack_prefix_kernel, chips),
        out_shape=[stack] * 2,
        in_specs=[SMEM, VMEM, VMEM],
        out_specs=[VMEM] * 2,
        name="pack_prefix",
    )(table, pool_keys, pool_values)
    got = swap(other, 1)
    messages = pl.pallas_call(
        functools.partial(merge_kernel, chips),
        out_shape=[message] * (chips - 1),
        in_specs=[VMEM] * 2,
        out_specs=[VMEM] * (chips - 1),
        name="merge",
    )(own, got)
    pages = [swap(messages[r - 1], 2 * r) for r in range(1, chips)]

    partial, stats = pl.pallas_call(
        functools.partial(fresh_kernel, group),
        grid=(KV_HEADS,),
        out_shape=[
            jax.ShapeDtypeStruct((span, HEADS * HEAD), f32),
            jax.ShapeDtypeStruct((KV_HEADS, span, HEAD), f32),
        ],
        in_specs=[
            SMEM,
            pl.BlockSpec((span, group * HEAD), lambda g: (0, g)),
            pl.BlockSpec((span, HEAD), lambda g: (0, g)),
            pl.BlockSpec((span, HEAD), lambda g: (0, g)),
        ],
        out_specs=[
            pl.BlockSpec((span, group * HEAD), lambda g: (0, g)),
            pl.BlockSpec((1, span, HEAD), lambda g: (g, 0, 0)),
        ],
        cost_estimate=pl.CostEstimate(
            flops=8 * span * span * HEADS * HEAD, bytes_accessed=8 * span * HEADS * HEAD, transcendentals=0
        ),
        name="fresh",
    )(new_len, queries, new_keys, new_values)

    relay = pl.pallas_call(
        functools.partial(exchange_pack_kernel, chips),
        out_shape=stack,
        in_specs=[VMEM] * chips,
        out_specs=VMEM,
        name="exchange_pack",
    )(*arrived)
    far = swap(relay, 1)
    pool_shape = jax.ShapeDtypeStruct(pool_keys.shape, bf16)
    pool_keys_out, pool_values_out = pl.pallas_call(
        functools.partial(scatter_kernel, chips),
        out_shape=[pool_shape] * 2,
        in_specs=[SMEM] + [VMEM] * (chips + 3),
        out_specs=[ANY] * 2,
        scratch_shapes=[
            pltpu.SMEM((slots,), jnp.int32),
            pltpu.SemaphoreType.DMA((4 * chips + 2 * slots,)),
        ],
        name="scatter",
    )(table, pool_keys, pool_values, *arrived, far)

    whole = lambda shape: pl.BlockSpec(shape, lambda g: (0,) * len(shape))
    attention_out = pl.pallas_call(
        functools.partial(prefix_kernel, chips, group),
        grid=(KV_HEADS,),
        out_shape=jax.ShapeDtypeStruct((span, HEADS * HEAD), bf16),
        in_specs=[
            SMEM,
            SMEM,
            SMEM,
            pl.BlockSpec((span, group * HEAD), lambda g: (0, g)),
            pl.BlockSpec((span, group * HEAD), lambda g: (0, g)),
            pl.BlockSpec((1, span, HEAD), lambda g: (g, 0, 0)),
        ]
        + [whole(stack.shape)] * 2
        + [whole(message.shape)] * (chips - 1),
        out_specs=pl.BlockSpec((span, group * HEAD), lambda g: (0, g)),
        scratch_shapes=[
            pltpu.VMEM((prefix_pages * rows, width), bf16),
            pltpu.VMEM((prefix_pages * rows, width), bf16),
        ],
        name="prefix",
    )(page_holder, prefix_len, new_len, queries, partial, stats, own, got, *pages)
    return (attention_out, pool_keys_out, pool_values_out)


def shards(*args):
    devices = lax.axis_size("seq")
    new_pages = args[9].shape[1]
    if devices == new_pages and devices >= 4 and devices & (devices - 1) == 0:
        return exchange_shards(*args)
    return general_shards(*args)


def solution(mesh):
    in_specs = (
        P(("groups", "seq"), None),
        P(("groups", "seq"), None),
        P(("groups", "seq"), None),
        P(("groups", "seq"), None, None),
        P(("groups", "seq"), None, None),
        P(("groups", "seq")),
        P(("groups", "seq")),
        P(("groups", "seq"), None),
        P(("groups", "seq"), None),
        P(("groups", "seq"), None),
        P(("groups", "seq"), None),
    )
    out_specs = (
        P(("groups", "seq"), None),
        P(("groups", "seq"), None, None),
        P(("groups", "seq"), None, None),
    )
    return jax.shard_map(shards, mesh=mesh, in_specs=in_specs, out_specs=out_specs, check_vma=False)
```

```python
import functools
import math

import jax
import jax.numpy as jnp
from jax import lax
from jax.experimental import pallas as pl
from jax.experimental.pallas import tpu as pltpu
from jax.sharding import PartitionSpec as P


HEADS = 32
KV_HEADS = 8
HEAD = 128


def score_block(query_block, key_slice, scaling):
    return (
        jnp.einsum("tgd,kd->tgk", query_block, key_slice, preferred_element_type=jnp.float32)
        * scaling
    )


def fresh_scores_all(queries, new_keys, fresh_live, scaling):
    group_size = HEADS // KV_HEADS
    span_rows = queries.shape[0]
    fresh_parts = []
    for head_group in range(KV_HEADS):
        first_col = head_group * group_size * HEAD
        query_block = queries[:, first_col : first_col + group_size * HEAD].reshape(
            span_rows, group_size, HEAD
        )
        key_slice = new_keys[:, head_group * HEAD : (head_group + 1) * HEAD]
        scores = score_block(query_block, key_slice, scaling)
        fresh_parts.append(jnp.where(fresh_live[:, None, :], scores, -jnp.inf))
    return fresh_parts


def general_shards(
    queries,
    new_keys,
    new_values,
    pool_keys,
    pool_values,
    prefix_len,
    new_len,
    page_holder,
    page_slot,
    new_holder,
    new_slot,
):
    devices = lax.axis_size("seq")
    pool_count = pool_keys.shape[0]
    page_rows = pool_keys.shape[1]
    kv_width = pool_keys.shape[2]
    span_rows = queries.shape[0]
    fresh_pages = span_rows // page_rows
    prefix_pages = page_holder.shape[1]
    group_size = HEADS // KV_HEADS
    scaling = 1.0 / math.sqrt(HEAD)
    peer_ids = jnp.arange(devices, dtype=jnp.int32)
    prefix_tokens = prefix_len[0]
    fresh_tokens = new_len[0]
    holders = page_holder[0]
    page_live = jnp.arange(prefix_pages, dtype=jnp.int32) * page_rows < prefix_tokens
    wanted = (holders[None, :] == peer_ids[:, None]) & page_live[None, :]
    request = jnp.sum(jnp.where(wanted, page_slot[0][None, :] + 1, 0), axis=1)
    token_pos = jnp.arange(span_rows, dtype=jnp.int32)
    row_keep = (token_pos < fresh_tokens)[:, None]
    fresh_live = (token_pos[None, :] <= token_pos[:, None]) & (token_pos[None, :] < fresh_tokens)
    kept_keys = jnp.where(row_keep, new_keys, 0).reshape(fresh_pages, page_rows * kv_width)
    kept_values = jnp.where(row_keep, new_values, 0).reshape(fresh_pages, page_rows * kv_width)
    target_hot = new_holder[0][None, :] == peer_ids[:, None]
    hot_matrix = target_hot.astype(jnp.bfloat16)
    out_keys = jnp.dot(hot_matrix, kept_keys, preferred_element_type=jnp.float32).astype(
        jnp.bfloat16
    )
    out_values = jnp.dot(hot_matrix, kept_values, preferred_element_type=jnp.float32).astype(
        jnp.bfloat16
    )
    out_slots = jnp.sum(jnp.where(target_hot, new_slot[0][None, :] + 1, 0), axis=1)
    slot_column = out_slots.astype(jnp.bfloat16)[:, None]
    incoming = (
        lax.all_to_all(
            request.astype(jnp.bfloat16)[:, None], "seq", split_axis=0, concat_axis=0, tiled=True
        ),
        lax.all_to_all(out_keys, "seq", split_axis=0, concat_axis=0, tiled=True),
        lax.all_to_all(out_values, "seq", split_axis=0, concat_axis=0, tiled=True),
        lax.all_to_all(slot_column, "seq", split_axis=0, concat_axis=0, tiled=True),
    )
    asked_slots = incoming[0][:, 0].astype(jnp.int32)
    returned = (incoming[1], incoming[2], incoming[3][:, 0].astype(jnp.int32))
    chosen = jnp.maximum(asked_slots - 1, 0)
    sending = (asked_slots > 0)[:, None, None]
    send_keys = jnp.where(sending, jnp.take(pool_keys, chosen, axis=0), 0)
    send_values = jnp.where(sending, jnp.take(pool_values, chosen, axis=0), 0)
    received_keys, received_values = (
        lax.all_to_all(send_keys, "seq", split_axis=0, concat_axis=0, tiled=True),
        lax.all_to_all(send_values, "seq", split_axis=0, concat_axis=0, tiled=True),
    )
    prefix_keys = jnp.take(received_keys, holders, axis=0).reshape(
        prefix_pages * page_rows, kv_width
    )
    prefix_values = jnp.take(received_values, holders, axis=0).reshape(
        prefix_pages * page_rows, kv_width
    )
    prefix_live = jnp.arange(prefix_pages * page_rows, dtype=jnp.int32) < prefix_tokens
    fresh_parts = fresh_scores_all(queries, new_keys, fresh_live, scaling)
    blocks = []
    for head_group in range(KV_HEADS):
        first_col = head_group * group_size * HEAD
        query_block = queries[:, first_col : first_col + group_size * HEAD].reshape(
            span_rows, group_size, HEAD
        )
        key_first = head_group * HEAD
        prefix_scores = score_block(
            query_block, prefix_keys[:, key_first : key_first + HEAD], scaling
        )
        prefix_scores = jnp.where(prefix_live[None, None, :], prefix_scores, -jnp.inf)
        fresh_part = fresh_parts[head_group]
        row_top = jnp.maximum(jnp.max(prefix_scores, axis=-1), jnp.max(fresh_part, axis=-1))[
            ..., None
        ]
        prefix_weights = jnp.exp(prefix_scores - row_top)
        fresh_weights = jnp.exp(fresh_part - row_top)
        weight_sum = jnp.sum(prefix_weights, axis=-1) + jnp.sum(fresh_weights, axis=-1)
        weighted = jnp.einsum(
            "tgk,kd->tgd",
            prefix_weights.astype(jnp.bfloat16),
            prefix_values[:, key_first : key_first + HEAD],
            preferred_element_type=jnp.float32,
        )
        weighted = weighted + jnp.einsum(
            "tgk,kd->tgd",
            fresh_weights.astype(jnp.bfloat16),
            new_values[:, key_first : key_first + HEAD],
            preferred_element_type=jnp.float32,
        )
        blocks.append((weighted / weight_sum[..., None]).reshape(span_rows, group_size * HEAD))
    attention_out = jnp.where(row_keep, jnp.concatenate(blocks, axis=1), 0.0).astype(jnp.bfloat16)
    slot_target = jnp.where(returned[2] > 0, returned[2] - 1, pool_count)
    pool_keys_out = pool_keys.at[slot_target].set(
        returned[0].reshape(devices, page_rows, kv_width), mode="drop"
    )
    pool_values_out = pool_values.at[slot_target].set(
        returned[1].reshape(devices, page_rows, kv_width), mode="drop"
    )
    return (attention_out, pool_keys_out, pool_values_out)


SMEM = pl.BlockSpec(memory_space=pltpu.SMEM)
VMEM = pl.BlockSpec(memory_space=pltpu.VMEM)
ANY = pl.BlockSpec(memory_space=pl.ANY)
LOG2E = 1.4426950408889634
VMEM_GRANT = 20 * 2**20


def in_vmem(value):
    return pltpu.with_memory_space_constraint(value, pltpu.VMEM)


def in_hbm(value):
    return pltpu.with_memory_space_constraint(value, pltpu.HBM)


def run_copies(pairs, sems):
    copies = [pltpu.make_async_copy(src, dst, sems.at[n]) for n, (src, dst) in enumerate(pairs)]
    for copy in copies:
        copy.start()
    for copy in copies:
        copy.wait()


def position():
    me = lax.axis_index("seq")
    return me // 2, me % 2


def pack_new_kernel(chips, *refs):
    new_len, tables, (keys, values), outs = refs[0], refs[1:5], refs[5:7], refs[7 : 7 + chips]
    table, where_page, sems, *small = refs[7 + chips :]
    run_copies(list(zip(tables, small)), sems)
    new_holder, new_slot, page_holder, page_slot = small
    chip, core = position()
    pages = new_holder.shape[1]
    rows = keys.shape[0] // pages
    for i in range(pages):
        where_page[new_holder[0, i]] = i
    pairs, places = [], []
    for r in range(chips):
        for side in range(2):
            start = pl.multiple_of(where_page[2 * (chip ^ r) + (core ^ side)] * rows, rows)
            places.append((r, side, start))
            pairs.append((keys.at[pl.ds(start, rows), :], outs[r].at[side, 0]))
            pairs.append((values.at[pl.ds(start, rows), :], outs[r].at[side, 1]))
    copies = [pltpu.make_async_copy(src, dst, sems.at[n]) for n, (src, dst) in enumerate(pairs)]
    for copy in copies:
        copy.start()
    row = lax.broadcasted_iota(jnp.int32, table.shape, 0)
    lane = lax.broadcasted_iota(jnp.int32, table.shape, 1)
    entry = jnp.zeros(table.shape, jnp.int32)
    for i in range(pages):
        entry = jnp.where((row == new_holder[0, i]) & (lane == 0), new_slot[0, i], entry)
    for j in range(page_holder.shape[1]):
        entry = jnp.where((row == page_holder[0, j]) & (lane == 1), page_slot[0, j] + 1, entry)
        entry = jnp.where((row == (page_holder[0, j] ^ 1)) & (lane == 2), page_slot[0, j] + 1, entry)
    table[...] = entry
    for copy in copies:
        copy.wait()
    live = new_len[0]
    token = lax.broadcasted_iota(jnp.int32, (rows, keys.shape[1]), 0)
    for r, side, start in places:

        @pl.when(start + rows > live)
        def _(r=r, side=side, start=start):
            keep = token + start < live
            for kv in range(2):
                outs[r][side, kv] = jnp.where(keep, outs[r][side, kv], 0)


def pack_prefix_kernel(chips, table, pool_keys, pool_values, near_keys, near_values, *rest):
    outs, sems = rest[:chips], rest[chips]
    chip, core = position()
    own = (pool_keys, pool_values)
    near = (near_keys, near_values)
    slots = [
        [jnp.maximum(table[2 * (chip ^ r) + core, 1 + side] - 1, 0) for side in range(2)]
        for r in range(chips)
    ]
    copies = [
        pltpu.make_async_copy(own[kv].at[slots[r][0]], outs[r].at[0, kv], sems.at[2 * r + kv])
        for r in range(chips)
        for kv in range(2)
    ]
    for copy in copies:
        copy.start()
    for r in range(chips):
        for kv in range(2):
            outs[r][1, kv] = near[kv][slots[r][1]]
    for copy in copies:
        copy.wait()


def relay_kernel(chips, *refs):
    out, sems = refs[chips:]
    run_copies([(refs[r].at[1], out.at[r]) for r in range(chips)], sems)


def scatter_kernel(chips, table, pool_keys, pool_values, *refs):
    near, far = refs[:chips], refs[chips]
    keys_out, values_out, taken, sems = refs[chips + 1 :]
    chip, core = position()
    slots = pool_keys.shape[0]
    for s in range(slots):
        taken[s] = 0
    pairs = []
    for r in range(chips):
        for side in range(2):
            slot = table[2 * (chip ^ r) + (core ^ side), 0]
            taken[slot] = 1
            page = near[r].at[0] if side == 0 else far.at[r]
            pairs.append((page.at[0], keys_out.at[slot]))
            pairs.append((page.at[1], values_out.at[slot]))
    copies = [pltpu.make_async_copy(src, dst, sems.at[n]) for n, (src, dst) in enumerate(pairs)]
    for copy in copies:
        copy.start()
    base = len(copies)

    def kept(s, action):
        for kv, (pool, dest) in enumerate(((pool_keys, keys_out), (pool_values, values_out))):

            @pl.when(taken[s] == 0)
            def _():
                action(pltpu.make_async_copy(pool.at[s], dest.at[s], sems.at[base + 2 * s + kv]))

    for s in range(slots):
        kept(s, lambda copy: copy.start())
    for copy in copies:
        copy.wait()
    for s in range(slots):
        kept(s, lambda copy: copy.wait())


def heads_of(queries, step, group, first, count):
    columns = [pl.multiple_of((step * group + h) * HEAD, HEAD) for h in range(group)]
    return jnp.concatenate(
        [queries[first : first + count, pl.ds(c, HEAD)] for c in columns], axis=0
    )


def key_scores(keys, queries):
    return lax.dot_general(
        keys, queries, (((1,), (1,)), ((), ())), preferred_element_type=jnp.float32
    )


def fresh_kernel(group, queries, keys, values, partial):
    half = keys.shape[0] // 2
    step = pl.program_id(0)
    scale = LOG2E / math.sqrt(HEAD)
    shape = (half, group * half)
    key_row = lax.broadcasted_iota(jnp.int32, shape, 0)
    token = lax.broadcasted_iota(jnp.int32, shape, 1) % half
    causal = key_row <= token
    first = pl.multiple_of(step * HEAD, HEAD)
    head_keys = keys[:, pl.ds(first, HEAD)]
    values_t = values[:, pl.ds(first, HEAD)].T
    for part in range(2):
        count = (part + 1) * half
        scores = key_scores(head_keys[0:count], heads_of(queries, step, group, part * half, half))
        pieces = [scores[0:half]] if part else []
        pieces.append(jnp.where(causal, scores[part * half :], -jnp.inf))
        top = functools.reduce(jnp.maximum, [jnp.max(p, axis=0, keepdims=True) for p in pieces])
        weights = [jnp.exp2((p - top) * scale) for p in pieces]
        total = functools.reduce(jnp.add, [jnp.sum(w, axis=0, keepdims=True) for w in weights])
        rounded = jnp.concatenate([w.astype(jnp.bfloat16) for w in weights], axis=0)
        partial[step, part, 0:HEAD] = jnp.dot(
            values_t[:, 0:count], rounded, preferred_element_type=jnp.float32
        )
        partial[step, part, HEAD : HEAD + 1] = top
        partial[step, part, HEAD + 1 : HEAD + 2] = total


def prefix_kernel(chips, group, holder, prefix_len, new_len, queries, partial, *refs):
    sources, (out, pages, sems) = refs[:chips], refs[chips:]
    chip, core = position()
    count, _, rows, _ = pages.shape
    step = pl.program_id(0)

    @pl.when(step == 0)
    def _():
        for j in range(count):
            source = holder[0, j]
            rel, side = (source // 2) ^ chip, (source % 2) ^ core
            for r in range(chips):

                @pl.when(rel == r)
                def _(r=r, j=j, side=side):
                    pltpu.make_async_copy(sources[r].at[side], pages.at[j], sems.at[j]).start()

        for j in range(count):
            pltpu.make_async_copy(sources[0].at[0], pages.at[j], sems.at[j]).wait()

    half = queries.shape[0] // 2
    tokens = count * rows
    scale = LOG2E / math.sqrt(HEAD)
    visible = lax.broadcasted_iota(jnp.int32, (tokens, group * half), 0) < prefix_len[0]
    lane_token = lax.broadcasted_iota(jnp.int32, (1, group * half), 1) % half
    first = pl.multiple_of(step * HEAD, HEAD)
    keys = pages[:, 0, :, pl.ds(first, HEAD)].reshape(tokens, HEAD)
    values_t = pages[:, 1, :, pl.ds(first, HEAD)].reshape(tokens, HEAD).T
    for part in range(2):
        scores = key_scores(keys, heads_of(queries, step, group, part * half, half))
        scores = jnp.where(visible, scores, -jnp.inf)
        fresh_top = partial[step, part, HEAD : HEAD + 1]
        fresh_total = partial[step, part, HEAD + 1 : HEAD + 2]
        top = jnp.maximum(jnp.max(scores, axis=0, keepdims=True), fresh_top)
        weights = jnp.exp2((scores - top) * scale)
        fade = jnp.exp2((fresh_top - top) * scale)
        total = jnp.sum(weights, axis=0, keepdims=True) + fresh_total * fade
        share = jnp.where(lane_token + part * half < new_len[0], 1.0 / total, 0.0)
        weighted = jnp.dot(
            values_t, weights.astype(jnp.bfloat16), preferred_element_type=jnp.float32
        )
        weighted = (weighted + partial[step, part, 0:HEAD] * fade) * share
        for h in range(group):
            out[part * half : (part + 1) * half, h * HEAD : (h + 1) * HEAD] = (
                weighted[:, h * half : (h + 1) * half].T.astype(jnp.bfloat16)
            )


def exchange_shards(
    queries,
    new_keys,
    new_values,
    pool_keys,
    pool_values,
    prefix_len,
    new_len,
    page_holder,
    page_slot,
    new_holder,
    new_slot,
):
    devices = lax.axis_size("seq")
    chips = devices // 2
    local = chips // 2
    group = HEADS // KV_HEADS
    span = queries.shape[0]
    slots, rows, width = pool_keys.shape
    prefix_pages = page_holder.shape[1]
    bf16, f32 = jnp.bfloat16, jnp.float32
    queries = in_vmem(queries)
    grant = dict(compiler_params=pltpu.CompilerParams(vmem_limit_bytes=VMEM_GRANT))
    dma = pltpu.SemaphoreType.DMA

    def swap(value, offset):
        return lax.ppermute(value, "seq", [(i, i ^ offset) for i in range(devices)])

    pair = pltpu.VMEM((2, 2, rows, width), bf16)
    tables = (new_holder, new_slot, page_holder, page_slot)
    *packed, table = pl.pallas_call(
        functools.partial(pack_new_kernel, chips),
        out_shape=[pair] * chips + [jax.ShapeDtypeStruct((devices, HEAD), jnp.int32)],
        in_specs=[SMEM] + [ANY] * 6,
        out_specs=[VMEM] * (chips + 1),
        scratch_shapes=[pltpu.SMEM((devices,), jnp.int32), dma((4 * chips,))]
        + [pltpu.SMEM(t.shape, jnp.int32) for t in tables],
        name="pack_new",
        **grant,
    )(new_len, *[in_hbm(t) for t in (*tables, new_keys, new_values)])
    arrived = [packed[0]] + [None] * (chips - 1)
    for r in [*range(local, chips), *range(1, local)]:
        arrived[r] = swap(packed[r], 2 * r)
    near_keys = swap(pool_keys, 1)
    near_values = swap(pool_values, 1)
    table = lax.all_to_all(table, "seq", split_axis=0, concat_axis=0, tiled=True)

    sources = pl.pallas_call(
        functools.partial(pack_prefix_kernel, chips),
        out_shape=[pair] * chips,
        in_specs=[SMEM, ANY, ANY, VMEM, VMEM],
        out_specs=[VMEM] * chips,
        scratch_shapes=[dma((2 * chips,))],
        name="pack_prefix",
        **grant,
    )(
        table,
        in_hbm(pool_keys),
        in_hbm(pool_values),
        in_vmem(near_keys),
        in_vmem(near_values),
    )
    pages = list(sources)
    for r in [*range(local, chips), *range(1, local)]:
        pages[r] = swap(sources[r], 2 * r)

    partial = pl.pallas_call(
        functools.partial(fresh_kernel, group),
        grid=(KV_HEADS,),
        out_shape=pltpu.VMEM((KV_HEADS, 2, HEAD + 8, group * span // 2), f32),
        in_specs=[VMEM] * 3,
        out_specs=VMEM,
        cost_estimate=pl.CostEstimate(
            flops=4 * span * span * HEADS * HEAD,
            bytes_accessed=8 * span * HEADS * HEAD,
            transcendentals=span * span * HEADS,
        ),
        name="fresh",
        **grant,
    )(queries, in_vmem(new_keys), in_vmem(new_values))

    arrived = [in_vmem(a) for a in arrived]
    relay = pl.pallas_call(
        functools.partial(relay_kernel, chips),
        out_shape=pltpu.VMEM((chips, 2, rows, width), bf16),
        in_specs=[VMEM] * chips,
        out_specs=VMEM,
        scratch_shapes=[dma((chips,))],
        name="relay",
        **grant,
    )(*arrived)
    far = swap(relay, 1)
    pool_shape = jax.ShapeDtypeStruct(pool_keys.shape, bf16)
    pool_keys_out, pool_values_out = pl.pallas_call(
        functools.partial(scatter_kernel, chips),
        out_shape=[pool_shape] * 2,
        in_specs=[SMEM] + [VMEM] * (chips + 3),
        out_specs=[ANY] * 2,
        scratch_shapes=[pltpu.SMEM((slots,), jnp.int32), dma((4 * chips + 2 * slots,))],
        name="scatter",
        **grant,
    )(table, in_vmem(pool_keys), in_vmem(pool_values), *arrived, in_vmem(far))

    attention_out = pl.pallas_call(
        functools.partial(prefix_kernel, chips, group),
        grid=(KV_HEADS,),
        out_shape=jax.ShapeDtypeStruct((span, HEADS * HEAD), bf16),
        in_specs=[SMEM] * 3 + [VMEM] * (chips + 2),
        out_specs=pl.BlockSpec((span, group * HEAD), lambda g: (0, g)),
        scratch_shapes=[pltpu.VMEM((prefix_pages, 2, rows, width), bf16), dma((prefix_pages,))],
        name="prefix",
        **grant,
    )(
        page_holder,
        prefix_len,
        new_len,
        queries,
        in_vmem(partial),
        *[in_vmem(p) for p in pages],
    )
    return (attention_out, pool_keys_out, pool_values_out)


def shards(*args):
    devices = lax.axis_size("seq")
    new_pages = args[9].shape[1]
    if devices == new_pages and devices >= 4 and devices & (devices - 1) == 0:
        return exchange_shards(*args)
    return general_shards(*args)


def solution(mesh):
    in_specs = (
        P(("groups", "seq"), None),
        P(("groups", "seq"), None),
        P(("groups", "seq"), None),
        P(("groups", "seq"), None, None),
        P(("groups", "seq"), None, None),
        P(("groups", "seq")),
        P(("groups", "seq")),
        P(("groups", "seq"), None),
        P(("groups", "seq"), None),
        P(("groups", "seq"), None),
        P(("groups", "seq"), None),
    )
    out_specs = (
        P(("groups", "seq"), None),
        P(("groups", "seq"), None, None),
        P(("groups", "seq"), None, None),
    )
    return jax.shard_map(
        shards, mesh=mesh, in_specs=in_specs, out_specs=out_specs, check_vma=False
    )
```

```python
import functools
import math

import jax
import jax.numpy as jnp
from jax import lax
from jax.experimental import pallas as pl
from jax.experimental.pallas import tpu as pltpu
from jax.sharding import PartitionSpec as P


HEADS = 32
KV_HEADS = 8
HEAD = 128


def score_block(query_block, key_slice, scaling):
    return (
        jnp.einsum("tgd,kd->tgk", query_block, key_slice, preferred_element_type=jnp.float32)
        * scaling
    )


def fresh_scores_all(queries, new_keys, fresh_live, scaling):
    group_size = HEADS // KV_HEADS
    span_rows = queries.shape[0]
    fresh_parts = []
    for head_group in range(KV_HEADS):
        first_col = head_group * group_size * HEAD
        query_block = queries[:, first_col : first_col + group_size * HEAD].reshape(
            span_rows, group_size, HEAD
        )
        key_slice = new_keys[:, head_group * HEAD : (head_group + 1) * HEAD]
        scores = score_block(query_block, key_slice, scaling)
        fresh_parts.append(jnp.where(fresh_live[:, None, :], scores, -jnp.inf))
    return fresh_parts


def general_shards(
    queries,
    new_keys,
    new_values,
    pool_keys,
    pool_values,
    prefix_len,
    new_len,
    page_holder,
    page_slot,
    new_holder,
    new_slot,
):
    devices = lax.axis_size("seq")
    pool_count = pool_keys.shape[0]
    page_rows = pool_keys.shape[1]
    kv_width = pool_keys.shape[2]
    span_rows = queries.shape[0]
    fresh_pages = span_rows // page_rows
    prefix_pages = page_holder.shape[1]
    group_size = HEADS // KV_HEADS
    scaling = 1.0 / math.sqrt(HEAD)
    peer_ids = jnp.arange(devices, dtype=jnp.int32)
    prefix_tokens = prefix_len[0]
    fresh_tokens = new_len[0]
    holders = page_holder[0]
    page_live = jnp.arange(prefix_pages, dtype=jnp.int32) * page_rows < prefix_tokens
    wanted = (holders[None, :] == peer_ids[:, None]) & page_live[None, :]
    request = jnp.sum(jnp.where(wanted, page_slot[0][None, :] + 1, 0), axis=1)
    token_pos = jnp.arange(span_rows, dtype=jnp.int32)
    row_keep = (token_pos < fresh_tokens)[:, None]
    fresh_live = (token_pos[None, :] <= token_pos[:, None]) & (token_pos[None, :] < fresh_tokens)
    kept_keys = jnp.where(row_keep, new_keys, 0).reshape(fresh_pages, page_rows * kv_width)
    kept_values = jnp.where(row_keep, new_values, 0).reshape(fresh_pages, page_rows * kv_width)
    target_hot = new_holder[0][None, :] == peer_ids[:, None]
    hot_matrix = target_hot.astype(jnp.bfloat16)
    out_keys = jnp.dot(hot_matrix, kept_keys, preferred_element_type=jnp.float32).astype(
        jnp.bfloat16
    )
    out_values = jnp.dot(hot_matrix, kept_values, preferred_element_type=jnp.float32).astype(
        jnp.bfloat16
    )
    out_slots = jnp.sum(jnp.where(target_hot, new_slot[0][None, :] + 1, 0), axis=1)
    slot_column = out_slots.astype(jnp.bfloat16)[:, None]
    incoming = (
        lax.all_to_all(
            request.astype(jnp.bfloat16)[:, None], "seq", split_axis=0, concat_axis=0, tiled=True
        ),
        lax.all_to_all(out_keys, "seq", split_axis=0, concat_axis=0, tiled=True),
        lax.all_to_all(out_values, "seq", split_axis=0, concat_axis=0, tiled=True),
        lax.all_to_all(slot_column, "seq", split_axis=0, concat_axis=0, tiled=True),
    )
    asked_slots = incoming[0][:, 0].astype(jnp.int32)
    returned = (incoming[1], incoming[2], incoming[3][:, 0].astype(jnp.int32))
    chosen = jnp.maximum(asked_slots - 1, 0)
    sending = (asked_slots > 0)[:, None, None]
    send_keys = jnp.where(sending, jnp.take(pool_keys, chosen, axis=0), 0)
    send_values = jnp.where(sending, jnp.take(pool_values, chosen, axis=0), 0)
    received_keys, received_values = (
        lax.all_to_all(send_keys, "seq", split_axis=0, concat_axis=0, tiled=True),
        lax.all_to_all(send_values, "seq", split_axis=0, concat_axis=0, tiled=True),
    )
    prefix_keys = jnp.take(received_keys, holders, axis=0).reshape(
        prefix_pages * page_rows, kv_width
    )
    prefix_values = jnp.take(received_values, holders, axis=0).reshape(
        prefix_pages * page_rows, kv_width
    )
    prefix_live = jnp.arange(prefix_pages * page_rows, dtype=jnp.int32) < prefix_tokens
    fresh_parts = fresh_scores_all(queries, new_keys, fresh_live, scaling)
    blocks = []
    for head_group in range(KV_HEADS):
        first_col = head_group * group_size * HEAD
        query_block = queries[:, first_col : first_col + group_size * HEAD].reshape(
            span_rows, group_size, HEAD
        )
        key_first = head_group * HEAD
        prefix_scores = score_block(
            query_block, prefix_keys[:, key_first : key_first + HEAD], scaling
        )
        prefix_scores = jnp.where(prefix_live[None, None, :], prefix_scores, -jnp.inf)
        fresh_part = fresh_parts[head_group]
        row_top = jnp.maximum(jnp.max(prefix_scores, axis=-1), jnp.max(fresh_part, axis=-1))[
            ..., None
        ]
        prefix_weights = jnp.exp(prefix_scores - row_top)
        fresh_weights = jnp.exp(fresh_part - row_top)
        weight_sum = jnp.sum(prefix_weights, axis=-1) + jnp.sum(fresh_weights, axis=-1)
        weighted = jnp.einsum(
            "tgk,kd->tgd",
            prefix_weights.astype(jnp.bfloat16),
            prefix_values[:, key_first : key_first + HEAD],
            preferred_element_type=jnp.float32,
        )
        weighted = weighted + jnp.einsum(
            "tgk,kd->tgd",
            fresh_weights.astype(jnp.bfloat16),
            new_values[:, key_first : key_first + HEAD],
            preferred_element_type=jnp.float32,
        )
        blocks.append((weighted / weight_sum[..., None]).reshape(span_rows, group_size * HEAD))
    attention_out = jnp.where(row_keep, jnp.concatenate(blocks, axis=1), 0.0).astype(jnp.bfloat16)
    slot_target = jnp.where(returned[2] > 0, returned[2] - 1, pool_count)
    pool_keys_out = pool_keys.at[slot_target].set(
        returned[0].reshape(devices, page_rows, kv_width), mode="drop"
    )
    pool_values_out = pool_values.at[slot_target].set(
        returned[1].reshape(devices, page_rows, kv_width), mode="drop"
    )
    return (attention_out, pool_keys_out, pool_values_out)


SMEM = pl.BlockSpec(memory_space=pltpu.SMEM)
VMEM = pl.BlockSpec(memory_space=pltpu.VMEM)
ANY = pl.BlockSpec(memory_space=pl.ANY)
LOG2E = 1.4426950408889634
VMEM_GRANT = 12 * 2**20


def in_vmem(value):
    return pltpu.with_memory_space_constraint(value, pltpu.VMEM)


def in_hbm(value):
    return pltpu.with_memory_space_constraint(value, pltpu.HBM)


def run_copies(pairs, sems):
    copies = [pltpu.make_async_copy(src, dst, sems.at[n]) for n, (src, dst) in enumerate(pairs)]
    for copy in copies:
        copy.start()
    for copy in copies:
        copy.wait()


def position():
    me = lax.axis_index("seq")
    return me // 2, me % 2


def pack_new_kernel(chips, *refs):
    local = chips // 2
    new_len, tables, wholes, outs = refs[0], refs[1:5], refs[5:7], refs[7 : 9 + local]
    table, where_page, sems, *scratch = refs[9 + local :]
    small, staged = scratch[:4], scratch[4:]
    sources, dests = [*tables, *wholes], [*small, *staged]
    copies = [pltpu.make_async_copy(a, b, sems.at[n]) for n, (a, b) in enumerate(zip(sources, dests))]
    for copy in copies:
        copy.start()
    for copy in copies[:4]:
        copy.wait()
    new_holder, new_slot, page_holder, page_slot = small
    chip, core = position()
    pages = new_holder.shape[1]
    rows = staged[0].shape[0] // pages
    for i in range(pages):
        where_page[new_holder[0, i]] = i
    row = lax.broadcasted_iota(jnp.int32, table.shape, 0)
    lane = lax.broadcasted_iota(jnp.int32, table.shape, 1)
    entry = jnp.zeros(table.shape, jnp.int32)
    for i in range(pages):
        entry = jnp.where((row == new_holder[0, i]) & (lane == 0), new_slot[0, i], entry)
    for j in range(page_holder.shape[1]):
        entry = jnp.where((row == page_holder[0, j]) & (lane == 1), page_slot[0, j] + 1, entry)
        entry = jnp.where((row == (page_holder[0, j] ^ 1)) & (lane == 2), page_slot[0, j] + 1, entry)
    table[...] = entry
    for copy in copies[4:]:
        copy.wait()
    live = new_len[0]
    token = lax.broadcasted_iota(jnp.int32, (rows, wholes[0].shape[1]), 0)
    for r in range(chips):
        for side in range(2):
            start = pl.multiple_of(where_page[2 * (chip ^ r) + (core ^ side)] * rows, rows)
            keep = token < live - start
            if r < local:
                out = outs[side].at[r]
            else:
                out = outs[2 + r - local].at[side]
            for kv in range(2):
                page = staged[kv][pl.ds(start, rows), :]
                out[kv] = jnp.where(keep, page, jnp.zeros_like(page))


def pack_prefix_kernel(chips, table, *refs):
    pools, news, outs = (refs[0:2], refs[2:4]), refs[4:6], refs[6:]
    local = chips // 2
    width = pools[0][0].shape[2]
    chip, core = position()
    for r in range(chips):
        for side in range(2):
            slot = jnp.maximum(table[2 * (chip ^ r) + core, 1 + side] - 1, 0)
            for kv in range(2):
                page = pools[side][kv].at[slot]
                if r < local:
                    outs[r][side, kv] = page[...]
                else:
                    outs[r][side, kv] = page[:, : width // 2]
                    outs[r + local][side, kv] = page[:, width // 2 :]
            if 0 < r < local:
                outs[r][2 + side] = news[side][r]


def stage_kernel(*refs):
    run_copies([(refs[0], refs[2]), (refs[1], refs[3])], refs[4])


def relay_kernel(*refs):
    for r, ref in enumerate(refs[:-1]):
        refs[-1][r] = ref[1]


def page_copies(table, pieces, outs, sems):
    chip, core = position()
    copies = []
    for r, side, page in pieces:
        slot = table[2 * (chip ^ r) + (core ^ side), 0]
        for kv in range(2):
            sem = sems.at[len(copies)]
            copies.append(pltpu.make_async_copy(page.at[kv], outs[kv].at[slot], sem))
    return copies


def scatter_copies(chips, table, pools, own, met, near, pages, far, outs, taken, kept, sems):
    local = chips // 2
    slots = pools[0].shape[0]
    for s in range(slots):
        taken[s] = 0
    for d in range(2 * chips):
        taken[table[d, 0]] = 1
    count = jnp.int32(0)
    for s in range(slots):
        kept[count] = s
        count = count + 1 - taken[s]
    pieces = [(0, 0, own.at[0]), (0, 1, met.at[0])]
    for r in range(1, local):
        pieces += [(r, side, pages[r].at[2 + side]) for side in range(2)]
    for n, ref in enumerate(near):
        pieces += [(local + n, 0, ref.at[0]), (local + n, 1, far.at[n])]
    copies = page_copies(table, pieces, outs, sems)
    for n in range(slots - 2 * chips):
        for kv in range(2):
            sem = sems.at[len(copies)]
            copies.append(pltpu.make_async_copy(pools[kv].at[kept[n]], outs[kv].at[kept[n]], sem))
    return copies


def heads_turned(queries, step, group, first, count):
    columns = [pl.multiple_of((step * group + h) * HEAD, HEAD) for h in range(group)]
    return jnp.concatenate(
        [queries[first : first + count, pl.ds(c, HEAD)].T for c in columns], axis=1
    )


def fresh_kernel(group, queries, keys, values, partial, turned):
    half = keys.shape[0] // 2
    step = pl.program_id(0)
    scale = LOG2E / math.sqrt(HEAD)
    shape = (half, group * half)
    key_row = lax.broadcasted_iota(jnp.int32, shape, 0)
    token = lax.broadcasted_iota(jnp.int32, shape, 1) % half
    causal = key_row <= token
    first = pl.multiple_of(step * HEAD, HEAD)
    head_keys = keys[:, pl.ds(first, HEAD)]
    values_t = values[:, pl.ds(first, HEAD)].T
    for part in range(2):
        count = (part + 1) * half
        heads = heads_turned(queries, step, group, part * half, half)
        turned[step, part] = heads
        scores = jnp.dot(head_keys[0:count], heads, preferred_element_type=jnp.float32)
        pieces = [scores[0:half]] if part else []
        pieces.append(jnp.where(causal, scores[part * half :], -jnp.inf))
        top = functools.reduce(jnp.maximum, [jnp.max(p, axis=0, keepdims=True) for p in pieces])
        weights = [jnp.exp2((p - top) * scale) for p in pieces]
        total = functools.reduce(jnp.add, [jnp.sum(w, axis=0, keepdims=True) for w in weights])
        rounded = jnp.concatenate([w.astype(jnp.bfloat16) for w in weights], axis=0)
        partial[step, part, 0:HEAD] = jnp.dot(
            values_t[:, 0:count], rounded, preferred_element_type=jnp.float32
        )
        partial[step, part, HEAD : HEAD + 1] = top
        partial[step, part, HEAD + 1 : HEAD + 2] = total


def prefix_kernel(chips, group, late, holder, prefix_len, new_len, turned, partial, *refs):
    local = chips // 2
    sources, refs = refs[:chips], refs[chips:]
    chip, core = position()
    copies = []
    if late:
        _, out, pages, staged, where_page, out_sems = refs
    else:
        table, *refs = refs
        pools, (own, met), near, far = refs[:2], refs[2:4], refs[4 : 4 + local], refs[4 + local]
        out, *pools_out, pages, staged, where_page, out_sems, taken, kept, sems = refs[5 + local :]
        copies = scatter_copies(
            chips, table, pools, own, met, near, sources, far, pools_out, taken, kept, sems
        )
        for copy in copies:
            copy.start()
    count = holder.shape[0]
    rows, width = pages.shape[2:]
    half = turned.shape[3] // group
    for d in range(2 * chips):
        where_page[d] = count
    for j in range(count):
        where_page[holder[j]] = j
    for r in range(chips):
        for side in range(2):
            page = sources[r].at[side]
            if r < local:
                page = page.at[:, :, pl.ds(late * width, width)]
            pages[where_page[2 * (chip ^ r) + (core ^ side)]] = page[...]
    tokens = count * rows
    scale = LOG2E / math.sqrt(HEAD)
    visible = lax.broadcasted_iota(jnp.int32, (tokens, group * half), 0) < prefix_len[0]
    lane_token = lax.broadcasted_iota(jnp.int32, (1, group * half), 1) % half
    heads = width // HEAD
    for place in range(heads):
        step = late * heads + place
        columns = slice(place * HEAD, (place + 1) * HEAD)
        keys = pages[0:count, 0, :, columns].reshape(tokens, HEAD)
        values_t = pages[0:count, 1, :, columns].reshape(tokens, HEAD).T
        for part in range(2):
            scores = jnp.dot(keys, turned[step, part], preferred_element_type=jnp.float32)
            scores = jnp.where(visible, scores, -jnp.inf)
            fresh_top = partial[step, part, HEAD : HEAD + 1]
            fresh_total = partial[step, part, HEAD + 1 : HEAD + 2]
            top = jnp.maximum(jnp.max(scores, axis=0, keepdims=True), fresh_top)
            weights = jnp.exp2((scores - top) * scale)
            fade = jnp.exp2((fresh_top - top) * scale)
            total = jnp.sum(weights, axis=0, keepdims=True) + fresh_total * fade
            share = jnp.where(lane_token + part * half < new_len[0], 1.0 / total, 0.0)
            weighted = jnp.dot(
                values_t, weights.astype(jnp.bfloat16), preferred_element_type=jnp.float32
            )
            weighted = ((weighted + partial[step, part, 0:HEAD] * fade) * share).astype(jnp.bfloat16)
            for h in range(group):
                column = (place * group + h) * HEAD
                staged[part * half : (part + 1) * half, column : column + HEAD] = weighted[
                    :, h * half : (h + 1) * half
                ].T
        size = group * HEAD
        source = staged.at[:, pl.ds(place * size, size)]
        dest = out.at[:, pl.ds(step * size, size)]
        copy = pltpu.make_async_copy(source, dest, out_sems.at[place])
        copy.start()
        copies.append(copy)
    for copy in copies:
        copy.wait()


def exchange_shards(
    queries,
    new_keys,
    new_values,
    pool_keys,
    pool_values,
    prefix_len,
    new_len,
    page_holder,
    page_slot,
    new_holder,
    new_slot,
):
    devices = lax.axis_size("seq")
    chips = devices // 2
    local = chips // 2
    group = HEADS // KV_HEADS
    span = queries.shape[0]
    slots, rows, width = pool_keys.shape
    prefix_pages = page_holder.shape[1]
    bf16, f32 = jnp.bfloat16, jnp.float32
    queries = in_vmem(queries)
    grant = dict(compiler_params=pltpu.CompilerParams(vmem_limit_bytes=VMEM_GRANT))
    dma = pltpu.SemaphoreType.DMA

    def swap(value, offset):
        return lax.ppermute(value, "seq", [(i, i ^ offset) for i in range(devices)])

    pair = pltpu.VMEM((2, 2, rows, width), bf16)
    double = pltpu.VMEM((4, 2, rows, width), bf16)
    part_pair = pltpu.VMEM((2, 2, rows, width // 2), bf16)
    stack = pltpu.VMEM((local, 2, rows, width), bf16)
    tables = (new_holder, new_slot, page_holder, page_slot)
    own, other, *packed, table = pl.pallas_call(
        functools.partial(pack_new_kernel, chips),
        out_shape=[stack] * 2
        + [pair] * local
        + [jax.ShapeDtypeStruct((devices, HEAD), jnp.int32)],
        in_specs=[SMEM] + [ANY] * 6,
        out_specs=[VMEM] * (local + 3),
        scratch_shapes=[pltpu.SMEM((devices,), jnp.int32), dma((6,))]
        + [pltpu.SMEM(t.shape, jnp.int32) for t in tables]
        + [pltpu.VMEM(new_keys.shape, bf16)] * 2,
        name="pack_new",
        **grant,
    )(new_len, *[in_hbm(t) for t in (*tables, new_keys, new_values)])
    near = [swap(m, 2 * r) for r, m in enumerate(packed, local)]
    own, met = in_vmem(own), in_vmem(swap(other, 1))
    near_keys = swap(pool_keys, 1)
    near_values = swap(pool_values, 1)
    staged = pl.pallas_call(
        stage_kernel,
        out_shape=[pltpu.VMEM(pool_keys.shape, bf16)] * 2,
        in_specs=[ANY] * 2,
        out_specs=[VMEM] * 2,
        scratch_shapes=[dma((2,))],
        name="stage",
        **grant,
    )(in_hbm(pool_keys), in_hbm(pool_values))
    staged = [in_vmem(p) for p in staged]
    table = lax.all_to_all(table, "seq", split_axis=0, concat_axis=0, tiled=True)

    sources = pl.pallas_call(
        functools.partial(pack_prefix_kernel, chips),
        out_shape=[double if 0 < r < local else pair for r in range(local)]
        + [part_pair] * (2 * local),
        in_specs=[SMEM] + [VMEM] * 6,
        out_specs=[VMEM] * (chips + local),
        name="pack_prefix",
        **grant,
    )(table, *staged, in_vmem(near_keys), in_vmem(near_values), own, met)
    near_pages = [sources[0]] + [swap(sources[r], 2 * r) for r in range(1, local)]
    near_pages = [in_vmem(p) for p in near_pages]
    far_pages = [
        [in_vmem(swap(sources[r + late * local], 2 * r)) for r in range(local, chips)]
        for late in range(2)
    ]

    partial, turned = pl.pallas_call(
        functools.partial(fresh_kernel, group),
        grid=(KV_HEADS,),
        out_shape=[
            pltpu.VMEM((KV_HEADS, 2, HEAD + 8, group * span // 2), f32),
            pltpu.VMEM((KV_HEADS, 2, HEAD, group * span // 2), bf16),
        ],
        in_specs=[VMEM] * 3,
        out_specs=[VMEM] * 2,
        cost_estimate=pl.CostEstimate(
            flops=4 * span * span * HEADS * HEAD,
            bytes_accessed=8 * span * HEADS * HEAD,
            transcendentals=span * span * HEADS,
        ),
        name="fresh",
        **grant,
    )(queries, in_vmem(new_keys), in_vmem(new_values))

    near = [in_vmem(n) for n in near]
    relay = pl.pallas_call(
        relay_kernel,
        out_shape=pltpu.VMEM((local, 2, rows, width), bf16),
        in_specs=[VMEM] * local,
        out_specs=VMEM,
        name="relay",
        **grant,
    )(*near)
    far = swap(relay, 1)
    pool_shape = jax.ShapeDtypeStruct(pool_keys.shape, bf16)

    out_shape = jax.ShapeDtypeStruct((span, HEADS * HEAD), bf16)
    scratch = [
        pltpu.VMEM((prefix_pages + 1, 2, rows, width // 2), bf16),
        pltpu.VMEM((span, HEADS * HEAD // 2), bf16),
        pltpu.SMEM((devices,), jnp.int32),
        dma((KV_HEADS // 2,)),
    ]
    scalars = (page_holder.reshape(prefix_pages), prefix_len, new_len)
    fresh = (in_vmem(turned), in_vmem(partial))
    early_out, pool_keys_out, pool_values_out = pl.pallas_call(
        functools.partial(prefix_kernel, chips, group, 0),
        out_shape=[out_shape, pool_shape, pool_shape],
        in_specs=[SMEM] * 3
        + [VMEM] * (chips + 2)
        + [SMEM]
        + [VMEM] * (local + 5),
        out_specs=[ANY] * 3,
        scratch_shapes=scratch
        + [
            pltpu.SMEM((slots,), jnp.int32),
            pltpu.SMEM((slots + 1,), jnp.int32),
            dma((4 * devices + 2 * slots,)),
        ],
        name="prefix0",
        **grant,
    )(*scalars, *fresh, *near_pages, *far_pages[0], table, *staged, own, met, *near, in_vmem(far))
    attention_out = pl.pallas_call(
        functools.partial(prefix_kernel, chips, group, 1),
        out_shape=out_shape,
        in_specs=[SMEM] * 3 + [VMEM] * (chips + 2) + [ANY],
        out_specs=ANY,
        scratch_shapes=scratch,
        input_output_aliases={chips + 5: 0},
        name="prefix1",
        **grant,
    )(*scalars, *fresh, *near_pages, *far_pages[1], early_out)
    return (attention_out, pool_keys_out, pool_values_out)


def shards(*args):
    devices = lax.axis_size("seq")
    new_pages = args[9].shape[1]
    if devices == new_pages and devices >= 4 and devices & (devices - 1) == 0:
        return exchange_shards(*args)
    return general_shards(*args)


def solution(mesh):
    in_specs = (
        P(("groups", "seq"), None),
        P(("groups", "seq"), None),
        P(("groups", "seq"), None),
        P(("groups", "seq"), None, None),
        P(("groups", "seq"), None, None),
        P(("groups", "seq")),
        P(("groups", "seq")),
        P(("groups", "seq"), None),
        P(("groups", "seq"), None),
        P(("groups", "seq"), None),
        P(("groups", "seq"), None),
    )
    out_specs = (
        P(("groups", "seq"), None),
        P(("groups", "seq"), None, None),
        P(("groups", "seq"), None, None),
    )
    return jax.shard_map(
        shards, mesh=mesh, in_specs=in_specs, out_specs=out_specs, check_vma=False
    )
```

```python
import functools
import math

import jax
import jax.numpy as jnp
from jax import lax
from jax.experimental import pallas as pl
from jax.experimental.pallas import tpu as pltpu
from jax.sharding import PartitionSpec as P


HEADS = 32
KV_HEADS = 8
HEAD = 128


def score_block(query_block, key_slice, scaling):
    return (
        jnp.einsum("tgd,kd->tgk", query_block, key_slice, preferred_element_type=jnp.float32)
        * scaling
    )


def fresh_scores_all(queries, new_keys, fresh_live, scaling):
    group_size = HEADS // KV_HEADS
    span_rows = queries.shape[0]
    fresh_parts = []
    for head_group in range(KV_HEADS):
        first_col = head_group * group_size * HEAD
        query_block = queries[:, first_col : first_col + group_size * HEAD].reshape(
            span_rows, group_size, HEAD
        )
        key_slice = new_keys[:, head_group * HEAD : (head_group + 1) * HEAD]
        scores = score_block(query_block, key_slice, scaling)
        fresh_parts.append(jnp.where(fresh_live[:, None, :], scores, -jnp.inf))
    return fresh_parts


def general_shards(
    queries,
    new_keys,
    new_values,
    pool_keys,
    pool_values,
    prefix_len,
    new_len,
    page_holder,
    page_slot,
    new_holder,
    new_slot,
):
    devices = lax.axis_size("seq")
    pool_count = pool_keys.shape[0]
    page_rows = pool_keys.shape[1]
    kv_width = pool_keys.shape[2]
    span_rows = queries.shape[0]
    fresh_pages = span_rows // page_rows
    prefix_pages = page_holder.shape[1]
    group_size = HEADS // KV_HEADS
    scaling = 1.0 / math.sqrt(HEAD)
    peer_ids = jnp.arange(devices, dtype=jnp.int32)
    prefix_tokens = prefix_len[0]
    fresh_tokens = new_len[0]
    holders = page_holder[0]
    page_live = jnp.arange(prefix_pages, dtype=jnp.int32) * page_rows < prefix_tokens
    wanted = (holders[None, :] == peer_ids[:, None]) & page_live[None, :]
    request = jnp.sum(jnp.where(wanted, page_slot[0][None, :] + 1, 0), axis=1)
    token_pos = jnp.arange(span_rows, dtype=jnp.int32)
    row_keep = (token_pos < fresh_tokens)[:, None]
    fresh_live = (token_pos[None, :] <= token_pos[:, None]) & (token_pos[None, :] < fresh_tokens)
    kept_keys = jnp.where(row_keep, new_keys, 0).reshape(fresh_pages, page_rows * kv_width)
    kept_values = jnp.where(row_keep, new_values, 0).reshape(fresh_pages, page_rows * kv_width)
    target_hot = new_holder[0][None, :] == peer_ids[:, None]
    hot_matrix = target_hot.astype(jnp.bfloat16)
    out_keys = jnp.dot(hot_matrix, kept_keys, preferred_element_type=jnp.float32).astype(
        jnp.bfloat16
    )
    out_values = jnp.dot(hot_matrix, kept_values, preferred_element_type=jnp.float32).astype(
        jnp.bfloat16
    )
    out_slots = jnp.sum(jnp.where(target_hot, new_slot[0][None, :] + 1, 0), axis=1)
    slot_column = out_slots.astype(jnp.bfloat16)[:, None]
    incoming = (
        lax.all_to_all(
            request.astype(jnp.bfloat16)[:, None], "seq", split_axis=0, concat_axis=0, tiled=True
        ),
        lax.all_to_all(out_keys, "seq", split_axis=0, concat_axis=0, tiled=True),
        lax.all_to_all(out_values, "seq", split_axis=0, concat_axis=0, tiled=True),
        lax.all_to_all(slot_column, "seq", split_axis=0, concat_axis=0, tiled=True),
    )
    asked_slots = incoming[0][:, 0].astype(jnp.int32)
    returned = (incoming[1], incoming[2], incoming[3][:, 0].astype(jnp.int32))
    chosen = jnp.maximum(asked_slots - 1, 0)
    sending = (asked_slots > 0)[:, None, None]
    send_keys = jnp.where(sending, jnp.take(pool_keys, chosen, axis=0), 0)
    send_values = jnp.where(sending, jnp.take(pool_values, chosen, axis=0), 0)
    received_keys, received_values = (
        lax.all_to_all(send_keys, "seq", split_axis=0, concat_axis=0, tiled=True),
        lax.all_to_all(send_values, "seq", split_axis=0, concat_axis=0, tiled=True),
    )
    prefix_keys = jnp.take(received_keys, holders, axis=0).reshape(
        prefix_pages * page_rows, kv_width
    )
    prefix_values = jnp.take(received_values, holders, axis=0).reshape(
        prefix_pages * page_rows, kv_width
    )
    prefix_live = jnp.arange(prefix_pages * page_rows, dtype=jnp.int32) < prefix_tokens
    fresh_parts = fresh_scores_all(queries, new_keys, fresh_live, scaling)
    blocks = []
    for head_group in range(KV_HEADS):
        first_col = head_group * group_size * HEAD
        query_block = queries[:, first_col : first_col + group_size * HEAD].reshape(
            span_rows, group_size, HEAD
        )
        key_first = head_group * HEAD
        prefix_scores = score_block(
            query_block, prefix_keys[:, key_first : key_first + HEAD], scaling
        )
        prefix_scores = jnp.where(prefix_live[None, None, :], prefix_scores, -jnp.inf)
        fresh_part = fresh_parts[head_group]
        row_top = jnp.maximum(jnp.max(prefix_scores, axis=-1), jnp.max(fresh_part, axis=-1))[
            ..., None
        ]
        prefix_weights = jnp.exp(prefix_scores - row_top)
        fresh_weights = jnp.exp(fresh_part - row_top)
        weight_sum = jnp.sum(prefix_weights, axis=-1) + jnp.sum(fresh_weights, axis=-1)
        weighted = jnp.einsum(
            "tgk,kd->tgd",
            prefix_weights.astype(jnp.bfloat16),
            prefix_values[:, key_first : key_first + HEAD],
            preferred_element_type=jnp.float32,
        )
        weighted = weighted + jnp.einsum(
            "tgk,kd->tgd",
            fresh_weights.astype(jnp.bfloat16),
            new_values[:, key_first : key_first + HEAD],
            preferred_element_type=jnp.float32,
        )
        blocks.append((weighted / weight_sum[..., None]).reshape(span_rows, group_size * HEAD))
    attention_out = jnp.where(row_keep, jnp.concatenate(blocks, axis=1), 0.0).astype(jnp.bfloat16)
    slot_target = jnp.where(returned[2] > 0, returned[2] - 1, pool_count)
    pool_keys_out = pool_keys.at[slot_target].set(
        returned[0].reshape(devices, page_rows, kv_width), mode="drop"
    )
    pool_values_out = pool_values.at[slot_target].set(
        returned[1].reshape(devices, page_rows, kv_width), mode="drop"
    )
    return (attention_out, pool_keys_out, pool_values_out)


SMEM = pl.BlockSpec(memory_space=pltpu.SMEM)
VMEM = pl.BlockSpec(memory_space=pltpu.VMEM)
ANY = pl.BlockSpec(memory_space=pl.ANY)
LOG2E = 1.4426950408889634
VMEM_GRANT = 12 * 2**20
EARLY_HEADS = 4


def in_vmem(value):
    return pltpu.with_memory_space_constraint(value, pltpu.VMEM)


def in_hbm(value):
    return pltpu.with_memory_space_constraint(value, pltpu.HBM)


def position():
    me = lax.axis_index("seq")
    return me // 2, me % 2


def pack_new_kernel(chips, *refs):
    local = chips // 2
    new_len, tables, wholes, pools = refs[0], refs[1:5], refs[5:7], refs[7:9]
    outs, (table, *pools_out) = refs[9 : 11 + local], refs[11 + local : 14 + local]
    where_page, sems, *scratch = refs[14 + local :]
    small, staged = scratch[:4], scratch[4:]
    sources, dests = [*tables, *wholes, *pools], [*small, *staged, *pools_out]
    copies = [pltpu.make_async_copy(a, b, sems.at[n]) for n, (a, b) in enumerate(zip(sources, dests))]
    for copy in copies:
        copy.start()
    for copy in copies[:4]:
        copy.wait()
    new_holder, new_slot, page_holder, page_slot = small
    chip, core = position()
    pages = new_holder.shape[1]
    rows = staged[0].shape[0] // pages
    for i in range(pages):
        where_page[new_holder[0, i]] = i
    row = lax.broadcasted_iota(jnp.int32, table.shape, 0)
    lane = lax.broadcasted_iota(jnp.int32, table.shape, 1)
    entry = jnp.zeros(table.shape, jnp.int32)
    for i in range(pages):
        entry = jnp.where((row == new_holder[0, i]) & (lane == 0), new_slot[0, i], entry)
    for j in range(page_holder.shape[1]):
        entry = jnp.where((row == page_holder[0, j]) & (lane == 1), page_slot[0, j] + 1, entry)
        entry = jnp.where((row == (page_holder[0, j] ^ 1)) & (lane == 2), page_slot[0, j] + 1, entry)
    table[...] = entry
    for copy in copies[4:6]:
        copy.wait()
    live = new_len[0]
    token = lax.broadcasted_iota(jnp.int32, (rows, wholes[0].shape[1]), 0)
    for r in range(chips):
        for side in range(2):
            start = pl.multiple_of(where_page[2 * (chip ^ r) + (core ^ side)] * rows, rows)
            keep = token < live - start
            if r < local:
                out = outs[side].at[r]
            else:
                out = outs[2 + r - local].at[side]
            for kv in range(2):
                page = staged[kv][pl.ds(start, rows), :]
                out[kv] = jnp.where(keep, page, jnp.zeros_like(page))
    for copy in copies[6:]:
        copy.wait()


def pack_prefix_kernel(chips, table, *refs):
    local = chips // 2
    cut = chips - 1
    pools, news, refs = (refs[0:2], refs[2:4]), refs[4:6], refs[6:]
    later, outs = refs[: chips - cut], refs[chips - cut :]
    width = pools[0][0].shape[2]
    early = EARLY_HEADS * HEAD
    chip, core = position()
    for r in range(chips):
        for side in range(2):
            slot = jnp.maximum(table[2 * (chip ^ r) + core, 1 + side] - 1, 0)
            for kv in range(2):
                page = pools[side][kv].at[slot]
                if r < local:
                    outs[r][side, kv] = page[...]
                else:
                    first = width if r >= cut else 0
                    outs[r][side, kv, :, first : first + early] = page[:, :early]
                    outs[r + local][side, kv] = page[:, early:]
            if 0 < r < local:
                outs[r][2 + side] = news[side][r]
            if r >= cut:
                outs[r][side, :, :, 0:width] = later[r - cut][side]


def relay_kernel(*refs):
    for r, ref in enumerate(refs[:-1]):
        refs[-1][r] = ref[1, :, :, 0 : refs[-1].shape[3]]


def page_copies(table, pieces, outs, sems):
    chip, core = position()
    copies = []
    for r, side, page in pieces:
        slot = table[2 * (chip ^ r) + (core ^ side), 0]
        for kv in range(2):
            copies.append(pltpu.make_async_copy(page.at[kv], outs[kv].at[slot], sems.at[kv]))
    return copies


def scatter_copies(chips, table, pools, own, met, near, pages, far, outs, taken, kept, sems):
    local = chips // 2
    slots = pools[0].shape[0]
    for s in range(slots):
        taken[s] = 0
    for d in range(2 * chips):
        taken[table[d, 0]] = 1
    count = jnp.int32(0)
    for s in range(slots):
        kept[count] = s
        count = count + 1 - taken[s]
    pieces = [(0, 0, own.at[0]), (0, 1, met.at[0])]
    for r in range(1, local):
        pieces += [(r, side, pages[r].at[2 + side]) for side in range(2)]
    for n, ref in enumerate(near):
        mine = ref.at[0, :, :, pl.ds(0, pools[0].shape[2])]
        pieces += [(local + n, 0, mine), (local + n, 1, far.at[n])]
    copies = page_copies(table, pieces, outs, sems)
    for n in range(slots - 2 * chips):
        for kv in range(2):
            source, dest = pools[kv].at[kept[n]], outs[kv].at[kept[n]]
            copies.append(pltpu.make_async_copy(source, dest, sems.at[kv]))
    for copy in copies:
        copy.start()
    return [pltpu.make_async_copy(pools[kv], outs[kv], sems.at[kv]) for kv in range(2)]


def heads_turned(queries, head, heads, first, count):
    columns = [pl.multiple_of((head + h) * HEAD, HEAD) for h in range(heads)]
    return jnp.concatenate(
        [queries[first : first + count, pl.ds(c, HEAD)].T for c in columns], axis=1
    )


def fresh_kernel(group, per_step, queries, keys, values, partial, turned):
    half = keys.shape[0] // 2
    scale = LOG2E / math.sqrt(HEAD)
    shape = (half, half)
    key_row = lax.broadcasted_iota(jnp.int32, shape, 0)
    token = lax.broadcasted_iota(jnp.int32, shape, 1) % half
    causal = key_row <= token
    for place in range(per_step):
        step = pl.program_id(0) * per_step + place
        first = pl.multiple_of(step * HEAD, HEAD)
        head_keys = keys[:, pl.ds(first, HEAD)]
        values_t = values[:, pl.ds(first, HEAD)].T
        for part in range(2):
            count = (part + 1) * half
            for h in range(group):
                lanes = slice(h * half, (h + 1) * half)
                heads = heads_turned(queries, step * group + h, 1, part * half, half)
                turned[step, part, :, lanes] = heads
                scores = jnp.dot(head_keys[0:count], heads, preferred_element_type=jnp.float32)
                pieces = [scores[0:half]] if part else []
                pieces.append(jnp.where(causal, scores[part * half :], -jnp.inf))
                top = functools.reduce(
                    jnp.maximum, [jnp.max(p, axis=0, keepdims=True) for p in pieces]
                )
                weights = [jnp.exp2((p - top) * scale) for p in pieces]
                total = functools.reduce(
                    jnp.add, [jnp.sum(w, axis=0, keepdims=True) for w in weights]
                )
                rounded = jnp.concatenate([w.astype(jnp.bfloat16) for w in weights], axis=0)
                partial[step, part, 0:HEAD, lanes] = jnp.dot(
                    values_t[:, 0:count], rounded, preferred_element_type=jnp.float32
                )
                partial[step, part, HEAD : HEAD + 1, lanes] = top
                partial[step, part, HEAD + 1 : HEAD + 2, lanes] = total


def prefix_kernel(chips, group, late, holder, prefix_len, new_len, turned, partial, *refs):
    local = chips // 2
    sources, refs = refs[:chips], refs[chips:]
    chip, core = position()
    copies = []
    if late:
        _, out, pages, staged, where_page, out_sems = refs
    else:
        table, *refs = refs
        pools, (own, met), near, far = refs[:2], refs[2:4], refs[4 : 4 + local], refs[4 + local]
        out, *pools_out, pages, staged, where_page, out_sems, taken, kept, sems = refs[5 + local :]
        copies = scatter_copies(
            chips, table, pools, own, met, near, sources, far, pools_out, taken, kept, sems
        )
    count = holder.shape[0]
    rows, width = pages.shape[2:]
    half = turned.shape[3] // group
    for d in range(2 * chips):
        where_page[d] = count
    for j in range(count):
        where_page[holder[j]] = j
    for r in range(chips):
        for side in range(2):
            first = late * EARLY_HEADS * HEAD if r < local else sources[r].shape[3] - width
            page = sources[r].at[side, :, :, pl.ds(first, width)]
            pages[where_page[2 * (chip ^ r) + (core ^ side)]] = page[...]
    places = pages.shape[0]
    for n in range(count + 1, places):
        pages[n] = pages[count]
    tokens = places * rows
    scale = LOG2E / math.sqrt(HEAD)
    visible = lax.broadcasted_iota(jnp.int32, (tokens, 2 * half), 0) < prefix_len[0]
    lane_token = lax.broadcasted_iota(jnp.int32, (1, 2 * half), 1) % half
    heads = width // HEAD
    for place in range(heads):
        step = late * EARLY_HEADS + place
        columns = slice(place * HEAD, (place + 1) * HEAD)
        keys = pages[:, 0, :, columns].reshape(tokens, HEAD)
        values_t = pages[:, 1, :, columns].reshape(tokens, HEAD).T
        for part in range(2):
            for h in range(0, group, 2):
                lanes = slice(h * half, (h + 2) * half)
                scores = jnp.dot(
                    keys, turned[step, part, :, lanes], preferred_element_type=jnp.float32
                )
                scores = jnp.where(visible, scores, -jnp.inf)
                fresh_top = partial[step, part, HEAD : HEAD + 1, lanes]
                fresh_total = partial[step, part, HEAD + 1 : HEAD + 2, lanes]
                top = jnp.maximum(jnp.max(scores, axis=0, keepdims=True), fresh_top)
                weights = jnp.exp2((scores - top) * scale)
                fade = jnp.exp2((fresh_top - top) * scale)
                total = jnp.sum(weights, axis=0, keepdims=True) + fresh_total * fade
                share = jnp.where(lane_token + part * half < new_len[0], 1.0 / total, 0.0)
                weighted = jnp.dot(
                    values_t, weights.astype(jnp.bfloat16), preferred_element_type=jnp.float32
                )
                weighted = (weighted + partial[step, part, 0:HEAD, lanes] * fade) * share
                weighted = weighted.astype(jnp.bfloat16)
                for k in range(2):
                    column = (place * group + h + k) * HEAD
                    staged[part * half : (part + 1) * half, column : column + HEAD] = weighted[
                        :, k * half : (k + 1) * half
                    ].T
        size = group * HEAD
        source = staged.at[:, pl.ds(place * size, size)]
        dest = out.at[:, pl.ds(step * size, size)]
        copy = pltpu.make_async_copy(source, dest, out_sems.at[place])
        copy.start()
        copies.append(copy)
    for copy in copies:
        copy.wait()


def exchange_shards(
    queries,
    new_keys,
    new_values,
    pool_keys,
    pool_values,
    prefix_len,
    new_len,
    page_holder,
    page_slot,
    new_holder,
    new_slot,
):
    devices = lax.axis_size("seq")
    chips = devices // 2
    local = chips // 2
    group = HEADS // KV_HEADS
    span = queries.shape[0]
    slots, rows, width = pool_keys.shape
    prefix_pages = page_holder.shape[1]
    bf16, f32 = jnp.bfloat16, jnp.float32
    queries = in_vmem(queries)
    grant = dict(compiler_params=pltpu.CompilerParams(vmem_limit_bytes=VMEM_GRANT))
    dma = pltpu.SemaphoreType.DMA

    def swap(value, offset):
        return lax.ppermute(value, "seq", [(i, i ^ offset) for i in range(devices)])

    pair = pltpu.VMEM((2, 2, rows, width), bf16)
    double = pltpu.VMEM((4, 2, rows, width), bf16)
    shares = (EARLY_HEADS, KV_HEADS - EARLY_HEADS)
    early, late = [pltpu.VMEM((2, 2, rows, n * HEAD), bf16) for n in shares]
    mixed = pltpu.VMEM((2, 2, rows, width + EARLY_HEADS * HEAD), bf16)
    cut = chips - 1
    stack = pltpu.VMEM((local, 2, rows, width), bf16)
    tables = (new_holder, new_slot, page_holder, page_slot)
    own, other, *packed, table, own_keys, own_values = pl.pallas_call(
        functools.partial(pack_new_kernel, chips),
        out_shape=[stack] * 2
        + [pair] * local
        + [jax.ShapeDtypeStruct((devices, HEAD), jnp.int32)]
        + [pltpu.VMEM(pool_keys.shape, bf16)] * 2,
        in_specs=[SMEM] + [ANY] * 8,
        out_specs=[VMEM] * (local + 5),
        scratch_shapes=[pltpu.SMEM((devices,), jnp.int32), dma((8,))]
        + [pltpu.SMEM(t.shape, jnp.int32) for t in tables]
        + [pltpu.VMEM(new_keys.shape, bf16)] * 2,
        name="pack_new",
        **grant,
    )(new_len, *[in_hbm(t) for t in (*tables, new_keys, new_values, pool_keys, pool_values)])
    staged = [in_vmem(own_keys), in_vmem(own_values)]
    near = [swap(packed[r - local], 2 * r) for r in range(local, cut)]
    own, met = in_vmem(own), in_vmem(swap(other, 1))
    near_keys = swap(pool_keys, 1)
    near_values = swap(pool_values, 1)
    table = lax.all_to_all(table, "seq", split_axis=0, concat_axis=0, tiled=True)

    sources = pl.pallas_call(
        functools.partial(pack_prefix_kernel, chips),
        out_shape=[double if 0 < r < local else pair for r in range(local)]
        + [early] * (cut - local)
        + [mixed] * (chips - cut)
        + [late] * local,
        in_specs=[SMEM] + [VMEM] * (6 + chips - cut),
        out_specs=[VMEM] * (chips + local),
        name="pack_prefix",
        **grant,
    )(table, *staged, in_vmem(near_keys), in_vmem(near_values), own, met, *[in_vmem(p) for p in packed[cut - local :]])
    near_pages = [sources[0]] + [swap(sources[r], 2 * r) for r in range(1, local)]
    near_pages = [in_vmem(p) for p in near_pages]
    far_pages = [
        [in_vmem(swap(sources[r + late * local], 2 * r)) for r in range(local, chips)]
        for late in range(2)
    ]
    near += far_pages[0][cut - local :]

    per_step = 4
    partial, turned = pl.pallas_call(
        functools.partial(fresh_kernel, group, per_step),
        grid=(KV_HEADS // per_step,),
        out_shape=[
            pltpu.VMEM((KV_HEADS, 2, HEAD + 8, group * span // 2), f32),
            pltpu.VMEM((KV_HEADS, 2, HEAD, group * span // 2), bf16),
        ],
        in_specs=[VMEM] * 3,
        out_specs=[VMEM] * 2,
        cost_estimate=pl.CostEstimate(
            flops=4 * span * span * HEADS * HEAD,
            bytes_accessed=8 * span * HEADS * HEAD,
            transcendentals=span * span * HEADS,
        ),
        name="fresh",
        **grant,
    )(queries, in_vmem(new_keys), in_vmem(new_values))

    near = [in_vmem(n) for n in near]
    relay = pl.pallas_call(
        relay_kernel,
        out_shape=pltpu.VMEM((local, 2, rows, width), bf16),
        in_specs=[VMEM] * local,
        out_specs=VMEM,
        name="relay",
        **grant,
    )(*near)
    far = swap(relay, 1)
    pool_shape = jax.ShapeDtypeStruct(pool_keys.shape, bf16)

    out_shape = jax.ShapeDtypeStruct((span, HEADS * HEAD), bf16)
    places = pl.cdiv((prefix_pages + 1) * rows, HEAD) * HEAD // rows
    scratch = [
        [
            pltpu.VMEM((places, 2, rows, n * HEAD), bf16),
            pltpu.VMEM((span, n * group * HEAD), bf16),
            pltpu.SMEM((devices,), jnp.int32),
            dma((n,)),
        ]
        for n in shares
    ]
    scalars = (page_holder.reshape(prefix_pages), prefix_len, new_len)
    fresh = (in_vmem(turned), in_vmem(partial))
    early_out, pool_keys_out, pool_values_out = pl.pallas_call(
        functools.partial(prefix_kernel, chips, group, 0),
        out_shape=[out_shape, pool_shape, pool_shape],
        in_specs=[SMEM] * 3
        + [VMEM] * (chips + 2)
        + [SMEM]
        + [VMEM] * (local + 5),
        out_specs=[ANY] * 3,
        scratch_shapes=scratch[0]
        + [
            pltpu.SMEM((slots,), jnp.int32),
            pltpu.SMEM((slots + 1,), jnp.int32),
            dma((2,)),
        ],
        name="prefix0",
        **grant,
    )(*scalars, *fresh, *near_pages, *far_pages[0], table, *staged, own, met, *near, in_vmem(far))
    attention_out = pl.pallas_call(
        functools.partial(prefix_kernel, chips, group, 1),
        out_shape=out_shape,
        in_specs=[SMEM] * 3 + [VMEM] * (chips + 2) + [ANY],
        out_specs=ANY,
        scratch_shapes=scratch[1],
        input_output_aliases={chips + 5: 0},
        name="prefix1",
        **grant,
    )(*scalars, *fresh, *near_pages, *far_pages[1], early_out)
    return (attention_out, pool_keys_out, pool_values_out)


def shards(*args):
    devices = lax.axis_size("seq")
    new_pages = args[9].shape[1]
    if devices == new_pages and devices >= 4 and devices & (devices - 1) == 0:
        return exchange_shards(*args)
    return general_shards(*args)


def solution(mesh):
    in_specs = (
        P(("groups", "seq"), None),
        P(("groups", "seq"), None),
        P(("groups", "seq"), None),
        P(("groups", "seq"), None, None),
        P(("groups", "seq"), None, None),
        P(("groups", "seq")),
        P(("groups", "seq")),
        P(("groups", "seq"), None),
        P(("groups", "seq"), None),
        P(("groups", "seq"), None),
        P(("groups", "seq"), None),
    )
    out_specs = (
        P(("groups", "seq"), None),
        P(("groups", "seq"), None, None),
        P(("groups", "seq"), None, None),
    )
    return jax.shard_map(
        shards, mesh=mesh, in_specs=in_specs, out_specs=out_specs, check_vma=False
    )
```
